512 devices in a mesh: fsdp: 64 (over z, x), tp: 8 (over y, core).
Axes of the slice: x: 4, y: 4, z: 16, core: 2. Of those that a mesh axis runs over, the one named last changes fastest.
Arguments:
- tokens: bfloat16 [2, 8192, 8192], P(None, 'fsdp', 'tp'), may hold values from -6 to 6
- frozen_weight: bfloat16 [8192, 2048], P('tp', 'fsdp'), may hold values from -0.0625 to 0.0625
- cotangent: bfloat16 [2, 8192, 2048], P(None, 'fsdp'), may hold values from -6 to 6
- block_adapter_index: int32 [2, 64], replicated, may hold values from 0 to 511
- down_weight: bfloat16 [512, 8192, 16], P(None, ('tp', 'fsdp')), may hold values from -0.0625 to 0.0625
- up_weight: bfloat16 [512, 16, 2048], P(None, None, ('tp', 'fsdp')), may hold values from -0.125 to 0.125
Outputs:
- key_value_output: bfloat16 [2, 8192, 2048], P(None, 'fsdp', 'tp')
- input_gradient: bfloat16 [2, 8192, 8192], P(None, 'fsdp', 'tp')
- grad_down: float32 [512, 8192, 16], P(None, ('tp', 'fsdp'))
- up_weight_gradient: float32 [512, 16, 2048], P(None, None, ('tp', 'fsdp'))
The draws below stay inside these ranges and needn't reach their ends.
Inputs may be any that keep to these rules, and one draw needn't show every extreme that they name: `block_adapter_index`: one adapter for each block of 128 rows of a microbatch.
All inputs are finite; a program needn't handle non-finite values.
Results may differ from the reference program's by a relative error of at most 0.005.
Values may be sent and summed in bfloat16 or wider, within the bound.
A program may use at most 64 MiB of HBM per device.

```python
import math
import jax
import jax.numpy as jnp
import numpy as np

MODEL_WIDTH = 8192
ADAPTER_RANK = 16
ADAPTER_TOTAL = 512
BLOCK = 128
MICROBATCH_COUNT = 2
KEY_VALUE_WIDTH = 2048
TOKEN_ROWS = 8192
BLOCKS_PER_BATCH = 64


def set_ends(result, rng, smallest, top_value):
    longest = result.shape.index(max(result.shape))
    spots = []
    for shift in (0, 1):
        where = [jax.random.randint(jax.random.fold_in(rng, axis), (), 0, length) for axis, length in enumerate(result.shape)]
        where[longest] = (where[longest] + shift) % result.shape[longest]
        spots.append(tuple(where))
    return result.at[spots[0]].set(smallest).at[spots[1]].set(top_value)


def level_of(own_key, dims, pieces, smallest, largest):
    def one(axis_at, parts):
        draws = jax.random.uniform(jax.random.fold_in(jax.random.fold_in(own_key, 6), axis_at), (parts,), jnp.float32, smallest / len(pieces), largest / len(pieces))
        return jnp.repeat(jnp.exp(draws), dims[axis_at] // parts).reshape((-1,) + (1,) * (len(dims) - axis_at - 1))

    factor_of = one(*pieces[0])
    for cut in pieces[1:]:
        factor_of = factor_of * one(*cut)
    return factor_of


def rank_bounds(amount, skew):
    weights = [(1 << 20) // math.isqrt(grade ** skew) + 1 for grade in range(1, amount + 1)]
    width = 1 + sum(weights) // (1 << 30)
    return np.cumsum(np.array([max(1, weight // width) for weight in weights]))


def skewed_ids(rng, shape, amount, lean):
    grid = rank_bounds(amount, lean)
    ticket = jax.random.randint(jax.random.fold_in(rng, 1), shape, 0, int(grid[amount - 1]))
    grade = jnp.searchsorted(jnp.asarray(grid, jnp.int32), ticket, side="right")
    return jax.random.permutation(jax.random.fold_in(rng, 2), amount)[grade].astype(jnp.int32)


def centred(rng, extent, deviation, reach, pieces=(), kind=jnp.bfloat16):
    values = jax.random.normal(rng, extent, jnp.float32) * deviation
    if len(pieces) > 0:
        values = level_of(rng, extent, pieces, -0.22, 0.18) * values
    return jnp.clip(values, min=-reach, max=reach).astype(kind)


def setup_inputs(seed: int = 0) -> dict:
    keys = jax.random.split(jax.random.key(seed), 7)
    return {
        "tokens": centred(keys[0], (MICROBATCH_COUNT, TOKEN_ROWS, MODEL_WIDTH), 1.0, 6.0, ((1, 64), (2, 8))),
        "frozen_weight": centred(keys[1], (MODEL_WIDTH, KEY_VALUE_WIDTH), MODEL_WIDTH ** -0.5, 0.0625, ((0, 8), (1, 64))),
        "cotangent": centred(keys[2], (MICROBATCH_COUNT, TOKEN_ROWS, KEY_VALUE_WIDTH), 1.0, 6.0, ((1, 64),)),
        "block_adapter_index": set_ends(skewed_ids(keys[3], (MICROBATCH_COUNT, BLOCKS_PER_BATCH), ADAPTER_TOTAL, 2), jax.random.fold_in(keys[3], 3), 0, ADAPTER_TOTAL - 1).astype(jnp.int32),
        "down_weight": centred(keys[4], (ADAPTER_TOTAL, MODEL_WIDTH, ADAPTER_RANK), MODEL_WIDTH ** -0.5, 0.0625, ((1, 512),)),
        "up_weight": centred(keys[5], (ADAPTER_TOTAL, ADAPTER_RANK, KEY_VALUE_WIDTH), KEY_VALUE_WIDTH ** -0.5, 0.125, ((2, 512),)),
    }


adapter_scale = 2.0


def reference(tokens, frozen_weight, cotangent, block_adapter_index, down_weight, up_weight):
    tok_matrix = tokens.reshape(MICROBATCH_COUNT * TOKEN_ROWS, MODEL_WIDTH)
    cot_matrix = cotangent.reshape(MICROBATCH_COUNT * TOKEN_ROWS, KEY_VALUE_WIDTH)
    frozen_key_value = jnp.dot(tok_matrix, frozen_weight, preferred_element_type=jnp.float32)
    frozen_input_gradient = jnp.dot(cot_matrix, frozen_weight.T, preferred_element_type=jnp.float32)
    tok_blocks = tokens.reshape(MICROBATCH_COUNT, BLOCKS_PER_BATCH, BLOCK, MODEL_WIDTH).astype(jnp.float32)
    gradient_blocks = cotangent.reshape(MICROBATCH_COUNT, BLOCKS_PER_BATCH, BLOCK, KEY_VALUE_WIDTH).astype(jnp.float32)
    down_weight_rows = jnp.take(down_weight, block_adapter_index, axis=0).astype(jnp.float32)
    up_weight_rows = jnp.take(up_weight, block_adapter_index, axis=0).astype(jnp.float32)
    low_rank = jnp.einsum("mnbd,mndr->mnbr", tok_blocks, down_weight_rows).astype(jnp.bfloat16)
    rank_gradient = (adapter_scale * jnp.einsum("fsvj,fsyj->fsvy", gradient_blocks, up_weight_rows)).astype(jnp.bfloat16)
    rank_wide_product = low_rank.astype(jnp.float32)
    wide_input_gradient = rank_gradient.astype(jnp.float32)
    adapter_key_value = (adapter_scale * jnp.einsum("elui,elis->elus", rank_wide_product, up_weight_rows)).astype(jnp.bfloat16)
    adapter_input_gradient = jnp.einsum("gwef,gwhf->gweh", wide_input_gradient, down_weight_rows).astype(jnp.bfloat16)
    key_value_output = (frozen_key_value.reshape(MICROBATCH_COUNT, TOKEN_ROWS, KEY_VALUE_WIDTH) + adapter_key_value.reshape(MICROBATCH_COUNT, TOKEN_ROWS, KEY_VALUE_WIDTH).astype(jnp.float32)).astype(jnp.bfloat16)
    input_gradient = (frozen_input_gradient.reshape(MICROBATCH_COUNT, TOKEN_ROWS, MODEL_WIDTH) + adapter_input_gradient.reshape(MICROBATCH_COUNT, TOKEN_ROWS, MODEL_WIDTH).astype(jnp.float32)).astype(jnp.bfloat16)
    down_tiles = jnp.einsum("mnbd,mnbr->mndr", tok_blocks, wide_input_gradient).reshape(MICROBATCH_COUNT * BLOCKS_PER_BATCH, MODEL_WIDTH, ADAPTER_RANK)
    up_weight_tiles = (adapter_scale * jnp.einsum("puai,puac->puic", rank_wide_product, gradient_blocks)).reshape(MICROBATCH_COUNT * BLOCKS_PER_BATCH, ADAPTER_RANK, KEY_VALUE_WIDTH)
    block_indices = block_adapter_index.reshape(-1).astype(jnp.int32)
    grad_down = jax.ops.segment_sum(down_tiles, block_indices, num_segments=ADAPTER_TOTAL)
    up_weight_gradient = jax.ops.segment_sum(up_weight_tiles, block_indices, num_segments=ADAPTER_TOTAL)
    return key_value_output, input_gradient, grad_down, up_weight_gradient
```

```python
import functools

import jax
import jax.numpy as jnp
from jax import lax
from jax.experimental import pallas as pl
from jax.experimental.pallas import tpu as pltpu
from jax.sharding import Mesh
from jax.sharding import PartitionSpec as P

MESH = pl.DeviceIdType.MESH
PLANE = ("z", "x")
TP = ("y", "c")
ALL = ("y", "c", "z", "x")

ZN, XN, TN = 16, 4, 8
FN = ZN * XN
BF = jnp.bfloat16
F32 = jnp.float32
NA = 2
LA = NA * 128
LB = 1024 - LA
ADAPT_AT = 3
TILES_AT = 5


def nt(a, b):
    return lax.dot_general(a, b, (((1,), (1,)), ((), ())), preferred_element_type=F32)


def nn(a, b):
    return jnp.dot(a, b, preferred_element_type=F32)


def iota(shape, dim):
    return lax.broadcasted_iota(jnp.int32, shape, dim)


def kernel(
    tok_ref, wt_ref, cot_ref, idx_ref, dn_ref, up_ref,
    kv_ref, ig_ref, gd_ref, gu_ref,
    wa, wb, acc, own_kv, rs_send, rs_recv, kvl, igl,
    onehot, sb32, sb1, sb2, rb32, rb1, rb2, d2t, up2, ar_send, ar_recv,
    s_loc, s_a, r_a, s_ax, r_ax, s_b, r_b, s_bx, r_bx, s_bf, r_bf,
    s_rs, r_rs, s_ar, r_ar, s_e, r_e, l_e,
):
    z, x = lax.axis_index("z"), lax.axis_index("x")
    tp = lax.axis_index("y") * 2 + lax.axis_index("c")
    f = z * XN + x

    def zmod(v):
        return lax.rem(v + 4 * ZN, ZN)

    def xmod(v):
        return lax.rem(v + 4 * XN, XN)

    def remote(src, dst, send, recv, device):
        return pltpu.make_async_remote_copy(
            src_ref=src, dst_ref=dst, send_sem=send, recv_sem=recv,
            device_id=device, device_id_type=MESH,
        )

    def plane_device(q):
        return {"z": lax.div(q, XN), "x": lax.rem(q, XN)}

    def tp_device(q):
        return {"y": lax.div(q, 2), "c": lax.rem(q, 2)}

    def rows_at(base, size):
        return pl.ds(pl.multiple_of(base, size), size)

    barrier = pltpu.get_barrier_semaphore()

    @pl.loop(1, FN)
    def _(p):
        pl.semaphore_signal(
            barrier, 1, device_id=plane_device(lax.rem(f + p, FN)), device_id_type=MESH
        )

    @pl.loop(1, TN)
    def _(t):
        pl.semaphore_signal(
            barrier, 1, device_id=tp_device(lax.rem(tp + t, TN)), device_id_type=MESH
        )

    own_rows = rows_at(f * 32, 32)
    own_a = pltpu.make_async_copy(wt_ref.at[:, 0:LA], wa.at[own_rows], s_loc.at[0])
    own_b = pltpu.make_async_copy(wt_ref.at[:, LA:1024], wb.at[own_rows], s_loc.at[1])
    own_a.start()
    own_b.start()

    zeros_up = jnp.zeros((64, FN), F32)
    sb32[...] = jnp.zeros_like(sb32)
    for m in range(2):
        pick = jnp.where(iota((512, FN), 0) == idx_ref[m : m + 1, :], 1.0, 0.0).astype(BF)
        onehot[m] = pick
        down = jnp.transpose(nn(dn_ref[...], pick))
        sb32[:, 2 * m, :] = down[:, 0:128]
        sb32[:, 2 * m + 1, :] = down[:, 128:256]
        up = jnp.concatenate([nn(up_ref[...], pick), zeros_up], axis=0)
        sb32[:, 4 + m, :] = jnp.transpose(up)
    sb1[...] = sb32[...].astype(BF)

    own_a.wait()
    own_b.wait()
    pl.semaphore_wait(barrier, FN - 1 + TN - 1)

    def exchange_start(src, dst, n):
        own = pltpu.make_async_copy(src.at[f], dst.at[f], l_e.at[n])
        own.start()

        @pl.loop(1, FN)
        def _(p):
            q = lax.rem(f + p, FN)
            remote(src.at[q], dst.at[f], s_e.at[n], r_e.at[n], plane_device(q)).start()

    def exchange_wait(src, dst, n):
        pltpu.make_async_copy(src.at[f], dst.at[f], l_e.at[n]).wait()
        remote(
            src.at[0 : FN - 1], dst.at[0 : FN - 1], s_e.at[n], r_e.at[n], plane_device(f)
        ).wait_recv()

    def exchange_drain(src, dst, n):
        remote(
            src.at[0 : FN - 1], dst.at[0 : FN - 1], s_e.at[n], r_e.at[n], plane_device(f)
        ).wait_send()

    def a_rows(d, k, xs):
        zz = zmod(z - k) if d == 0 else zmod(z + k)
        return rows_at(zz * 128 + xs * 32, 32)

    def b_rows(d, k):
        return a_rows(d, k, x)

    def ring_device(d):
        return {"z": zmod(z + 1) if d == 0 else zmod(z - 1)}

    def a_copy(d, k, xs):
        rows = wa.at[a_rows(d, k, xs)]
        return remote(rows, rows, s_a.at[d, k, xs], r_a.at[d, k + 1, xs], ring_device(d))

    def a_wait(d, k, xs):
        rows = wa.at[a_rows(d, k, xs)]
        remote(rows, rows, s_a.at[d, 0, xs], r_a.at[d, k, xs], ring_device(d)).wait_recv()

    def ax_copy(i):
        rows = wa.at[own_rows]
        return remote(rows, rows, s_ax.at[i], r_ax.at[x], {"x": xmod(x + i)})

    def ax_wait(xs):
        rows = wa.at[a_rows(0, 0, xs)]
        remote(rows, rows, s_ax.at[1], r_ax.at[xs], {"x": xmod(x + 1)}).wait_recv()

    def b_copy(d, k):
        rows = wb.at[b_rows(d, k)]
        return remote(rows, rows, s_b.at[d, k], r_b.at[d, k + 1], ring_device(d))

    def b_wait(d, k):
        rows = wb.at[b_rows(d, k)]
        remote(rows, rows, s_b.at[d, 0], r_b.at[d, k], ring_device(d)).wait_recv()

    def b_half(d, k):
        zz = zmod(z - k) if d == 0 else zmod(z + k)
        return wb.at[rows_at(zz * 128 + x * 32 + 16 * d, 16)]

    def b_half_copy(d):
        rows = b_half(d, 7)
        return remote(rows, rows, s_b.at[d, 7], r_b.at[d, 8], ring_device(d))

    def b_half_wait(d):
        rows = b_half(d, 8)
        remote(rows, rows, s_b.at[d, 7], r_b.at[d, 8], ring_device(d)).wait_recv()

    def slot(d, k):
        return k if d == 0 else 8 + k

    def x_device(side):
        return {"x": xmod(x + 1)} if side == 0 else {"x": xmod(x - 1)}

    def bx_rows(d, k, from_x):
        return wb.at[a_rows(d, k, from_x)]

    def bx_copy(side, d, k):
        rows = bx_rows(d, k, x)
        n = slot(d, k)
        return remote(rows, rows, s_bx.at[side, n], r_bx.at[side, n], x_device(side))

    def bx_wait(side, d, k):
        n = slot(d, k)
        rows = bx_rows(d, k, xmod(x - 1) if side == 0 else xmod(x + 1))
        remote(rows, rows, s_bx.at[side, n], r_bx.at[side, n], x_device(side)).wait_recv()

    def bf_rows(side, d, k, from_x):
        zz = zmod(z - k) if d == 0 else zmod(z + k)
        return wb.at[rows_at(zz * 128 + from_x * 32 + 16 * side, 16)]

    def bf_copy(side, d, k):
        n = slot(d, k)
        rows = bf_rows(side, d, k, xmod(x - 1) if side == 0 else xmod(x + 1))
        return remote(rows, rows, s_bf.at[side, n], r_bf.at[side, n], x_device(side))

    def bf_wait(side, d, k):
        n = slot(d, k)
        rows = bf_rows(side, d, k, xmod(x + 2))
        remote(rows, rows, s_bf.at[side, n], r_bf.at[side, n], x_device(side)).wait_recv()

    def spread(d, k):
        for side in range(2):
            bx_copy(side, d, k).start()

    def forward_x(d, k):
        for side in range(2):
            bx_wait(side, d, k)
            bf_copy(side, d, k).start()

    def complete_x(d, k):
        for side in range(2):
            bf_wait(side, d, k)

    def rs_copy(c):
        return remote(
            rs_send.at[c], rs_recv.at[tp], s_rs.at[c], r_rs.at[tp], tp_device(c)
        )

    def block(k):
        odd = lax.rem(z + k, 2)
        start = zmod(jnp.where(odd == 1, z + k - 1, z - k))
        c = lax.div(start, 2)
        rows = rows_at(c * 256, 256)
        w_a, w_b = wa[rows, :], wb[rows, :]
        part = nt(tok_ref[:, 0:LA], w_a) + nt(tok_ref[:, LA:1024], w_b)

        @pl.when(c == tp)
        def _():
            own_kv[...] = part

        @pl.when(c != tp)
        def _():
            rs_send[c] = part.astype(BF)
            rs_copy(c).start()

        cot = cot_ref[:, rows]
        acc[:, 0:LA] += nn(cot, w_a)
        acc[:, LA:1024] += nn(cot, w_b)

    rep = jnp.where(lax.div(iota((FN, 1024), 1), 16) == iota((FN, 1024), 0), 1.0, 0.0).astype(BF)
    rep_up = jnp.where(lax.div(iota((FN, 256), 1), 4) == iota((FN, 256), 0), 1.0, 0.0).astype(BF)
    lane16 = lax.rem(iota((16, 1024), 1), 16)
    lane4 = lax.rem(iota((16, 256), 1), 4)
    first = iota((16, 256), 1) < 128
    cot_cols = pl.ds(pl.multiple_of(tp * 256, 256), 256)

    def arrived(m):
        down = jnp.concatenate(
            [jnp.transpose(rb32[:, 2 * m, :]), jnp.transpose(rb32[:, 2 * m + 1, :])], axis=0
        )
        up = jnp.transpose(rb32[:, 4 + m, :])[0:64, :]
        return down.astype(BF), up.astype(BF)

    def folded(value):
        return jnp.where(first, value[0:16], value[16:32])

    def unfolded(value):
        return jnp.concatenate(
            [jnp.where(first, value, 0.0), jnp.where(first, 0.0, value)], axis=0
        )

    def adapters():
        exchange_wait(sb1, rb1, 0)
        rb32[...] = rb1[...].astype(F32)
        for m in range(2):
            down, up = arrived(m)
            wide = nn(down, rep)
            total = jnp.zeros((16, 1024), F32)
            for d in range(16):
                total = jnp.where(lane16 == d, wide[16 * d : 16 * d + 16], total)
            d2t[16 * m : 16 * m + 16] = total.astype(BF)
            wide = nn(up, rep_up)
            total = jnp.zeros((16, 256), F32)
            for d in range(4):
                total = jnp.where(lane4 == d, wide[16 * d : 16 * d + 16], total)
            up2[16 * m : 16 * m + 16] = total.astype(BF)
        ar_send[0:16] = folded(nt(d2t[...], tok_ref[...]))
        ar_send[16:32] = 2.0 * folded(nt(up2[...], cot_ref[:, cot_cols]))
        ar_recv[tp] = ar_send[...]

        @pl.loop(1, TN)
        def _(t):
            ar_copy(t).start()

    def ar_copy(t):
        q = lax.rem(tp + t, TN)
        return remote(ar_send, ar_recv.at[tp], s_ar.at[t], r_ar.at[tp], tp_device(q))

    def tiles():
        @pl.loop(1, TN)
        def _(t):
            q = lax.rem(tp + t, TN)
            remote(ar_send, ar_recv.at[q], s_ar.at[t], r_ar.at[q], tp_device(q)).wait_recv()

        total = ar_recv[0]
        for q in range(1, TN):
            total = total + ar_recv[q]
        low = unfolded(total[0:16].astype(BF).astype(F32))
        back = unfolded(total[16:32].astype(BF).astype(F32))
        low_t, back_t = jnp.transpose(low).astype(BF), jnp.transpose(back).astype(BF)
        low, back = low.astype(BF), back.astype(BF)
        down = nn(back, tok_ref[...])
        up = 2.0 * nn(low, cot_ref[:, cot_cols])
        zeros = jnp.zeros((64, 256), BF)
        for m in range(2):
            mine = down[16 * m : 16 * m + 16]
            wide = jnp.concatenate(
                [jnp.where(lane16 == d, mine, 0.0).astype(BF) for d in range(16)], axis=0
            )
            packed = jnp.transpose(nt(wide, rep))
            sb32[:, 2 * m, :] = packed[:, 0:128]
            sb32[:, 2 * m + 1, :] = packed[:, 128:256]
            mine = up[16 * m : 16 * m + 16]
            wide = jnp.concatenate(
                [jnp.where(lane4 == d, mine, 0.0).astype(BF) for d in range(4)] + [zeros], axis=0
            )
            sb32[:, 4 + m, :] = jnp.transpose(nt(wide, rep_up))
        sb2[...] = sb32[...].astype(BF)
        exchange_start(sb2, rb2, 1)
        kvl[...] = (2.0 * nn(low_t, up2[...])).astype(BF)
        igl[...] = nn(back_t, d2t[...]).astype(BF)

    def gradients():
        exchange_wait(sb2, rb2, 1)
        rb32[...] = rb2[...].astype(F32)
        down0, up0 = arrived(0)
        down1, up1 = arrived(1)
        gd_ref[...] = nt(down0, onehot[0]) + nt(down1, onehot[1])
        gu_ref[...] = nt(up0, onehot[0]) + nt(up1, onehot[1])

    for i in range(1, XN):
        ax_copy(i).start()
    for d in range(2):
        b_copy(d, 0).start()
        a_copy(d, 0, x).start()
    spread(0, 0)
    exchange_start(sb1, rb1, 0)
    acc[...] = jnp.zeros_like(acc)
    for i in range(1, XN):
        xs = xmod(x + i)
        ax_wait(xs)
        for d in range(2):
            a_copy(d, 0, xs).start()
    forward_x(0, 0)
    complete_x(0, 0)

    @pl.loop(1, 8)
    def _(k):
        for d in range(2):
            for i in range(XN):
                xs = xmod(x + i)
                a_wait(d, k, xs)

                @pl.when((k < 7) | (lax.div(xs, 2) == d))
                def _():
                    a_copy(d, k, xs).start()

            b_wait(d, k)

            @pl.when(k < 7)
            def _():
                b_copy(d, k).start()

            @pl.when(k == 7)
            def _():
                b_half_copy(d).start()

            spread(d, k)

        @pl.when(k >= 2)
        def _():
            for d in range(2):
                forward_x(d, k - 1)

        @pl.when(k >= 3)
        def _():
            for d in range(2):
                complete_x(d, k - 2)
            block(k - 2)

        @pl.when(k == ADAPT_AT)
        def _():
            adapters()

        @pl.when(k == TILES_AT)
        def _():
            tiles()

    for d in range(2):
        for h in range(2):
            a_wait(d, 8, 2 * d + h)
        b_half_wait(d)
    spread(0, 8)
    for d in range(2):
        forward_x(d, 7)
    for d in range(2):
        complete_x(d, 6)
    block(6)
    forward_x(0, 8)
    for d in range(2):
        complete_x(d, 7)
    block(7)
    gradients()
    complete_x(0, 8)
    block(8)
    ig_ref[...] = (acc[...] + igl[...].astype(F32)).astype(BF)

    total = own_kv[...]
    for t in range(1, TN):
        q = lax.rem(tp + t, TN)
        remote(
            rs_send.at[q], rs_recv.at[q], s_rs.at[q], r_rs.at[q], tp_device(q)
        ).wait_recv()
        total = total + rs_recv[q].astype(F32)
    kv_ref[...] = (total + kvl[...].astype(F32)).astype(BF)

    exchange_drain(sb1, rb1, 0)
    exchange_drain(sb2, rb2, 1)
    for i in range(1, XN):
        ax_copy(i).wait_send()

    @pl.loop(1, TN)
    def _(t):
        ar_copy(t).wait_send()
        rs_copy(lax.rem(tp + t, TN)).wait_send()

    for d in range(2):

        @pl.loop(0, 7)
        def _(k):
            for xs in range(XN):
                a_copy(d, k, xs).wait_send()
            b_copy(d, k).wait_send()

        for h in range(2):
            a_copy(d, 7, 2 * d + h).wait_send()
        b_half_copy(d).wait_send()
    for side in range(2):

        @pl.loop(0, 9)
        def _(k):
            bx_copy(side, 0, k).wait_send()
            bf_copy(side, 0, k).wait_send()

        @pl.loop(1, 8)
        def _(k):
            bx_copy(side, 1, k).wait_send()
            bf_copy(side, 1, k).wait_send()


def fused(tok, wt, cot, idx, dn, up):
    dma = pltpu.SemaphoreType.DMA
    vmem = pl.BlockSpec(memory_space=pltpu.VMEM)
    return pl.pallas_call(
        kernel,
        out_shape=(
            jax.ShapeDtypeStruct((256, 256), BF),
            jax.ShapeDtypeStruct((256, 1024), BF),
            jax.ShapeDtypeStruct((256, 512), F32),
            jax.ShapeDtypeStruct((64, 512), F32),
        ),
        in_specs=[vmem] * 6,
        out_specs=[vmem] * 4,
        scratch_shapes=[
            pltpu.VMEM((2048, LA), BF),
            pltpu.VMEM((2048, LB), BF),
            pltpu.VMEM((256, 1024), F32),
            pltpu.VMEM((256, 256), F32),
            pltpu.VMEM((TN, 256, 256), BF),
            pltpu.VMEM((TN, 256, 256), BF),
            pltpu.VMEM((256, 256), BF),
            pltpu.VMEM((256, 1024), BF),
            pltpu.VMEM((2, 512, FN), BF),
            pltpu.VMEM((FN, 8, 128), F32),
            pltpu.VMEM((FN, 8, 128), BF),
            pltpu.VMEM((FN, 8, 128), BF),
            pltpu.VMEM((FN, 8, 128), F32),
            pltpu.VMEM((FN, 8, 128), BF),
            pltpu.VMEM((FN, 8, 128), BF),
            pltpu.VMEM((32, 1024), BF),
            pltpu.VMEM((32, 256), BF),
            pltpu.VMEM((32, 256), F32),
            pltpu.VMEM((TN, 32, 256), F32),
            dma((2,)),
            dma((2, 8, XN)),
            dma((2, 9, XN)),
            dma((XN,)),
            dma((XN,)),
            dma((2, 8)),
            dma((2, 9)),
            dma((2, 16)),
            dma((2, 16)),
            dma((2, 16)),
            dma((2, 16)),
            dma((TN,)),
            dma((TN,)),
            dma((TN,)),
            dma((TN,)),
            dma((2,)),
            dma((2,)),
            dma((2,)),
        ],
        compiler_params=pltpu.CompilerParams(
            collective_id=0, has_side_effects=True, vmem_limit_bytes=56 << 20
        ),
    )(tok, wt, cot, idx, dn, up)


def local(tokens, frozen_weight, cotangent, block_adapter_index, down_weight, up_weight):
    tok = tokens.reshape(256, 1024)
    cot = cotangent.reshape(256, 2048)
    wt = frozen_weight.T
    dn = down_weight.transpose(1, 2, 0).reshape(256, 512)
    up = up_weight.transpose(2, 1, 0).reshape(64, 512)
    kv, ig, gd, gu = fused(tok, wt, cot, block_adapter_index, dn, up)
    return (
        kv.reshape(2, 128, 256),
        ig.reshape(2, 128, 1024),
        gd.reshape(16, 16, 512).transpose(2, 0, 1),
        gu.reshape(4, 16, 512).transpose(2, 1, 0),
    )


def solution(mesh):
    finer = Mesh(mesh.devices.reshape(ZN, XN, 4, 2), ("z", "x", "y", "c"))
    return jax.shard_map(
        local,
        mesh=finer,
        in_specs=(
            P(None, PLANE, TP),
            P(TP, PLANE),
            P(None, PLANE, None),
            P(),
            P(None, ALL, None),
            P(None, None, ALL),
        ),
        out_specs=(
            P(None, PLANE, TP),
            P(None, PLANE, TP),
            P(None, ALL, None),
            P(None, None, ALL),
        ),
        check_vma=False,
    )
```

```python
import functools

import jax
import jax.numpy as jnp
from jax import lax
from jax.experimental import pallas as pl
from jax.experimental.pallas import tpu as pltpu
from jax.sharding import Mesh
from jax.sharding import PartitionSpec as P

MESH = pl.DeviceIdType.MESH
PLANE = ("z", "x")
TP = ("y", "c")
ALL = ("y", "c", "z", "x")

ZN, XN, TN = 16, 4, 8
FN = ZN * XN
BF = jnp.bfloat16
F32 = jnp.float32
NA = 2
LA = NA * 128
LB = 1024 - LA
ADAPT_AT = 4
TILES_AT = 6


def nt(a, b):
    return lax.dot_general(a, b, (((1,), (1,)), ((), ())), preferred_element_type=F32)


def nn(a, b):
    return jnp.dot(a, b, preferred_element_type=F32)


def iota(shape, dim):
    return lax.broadcasted_iota(jnp.int32, shape, dim)


def arrived(ref, m):
    down = [jnp.transpose(ref[:, 2 * m + h, :]) for h in range(2)]
    up = jnp.transpose(ref[:, 4 + m, :])[0:64, :]
    return jnp.concatenate(down, axis=0).astype(BF), up.astype(BF)


def finish(kv_in, ig_in, got_in, idx_ref, kv_ref, ig_ref, gd_ref, gu_ref, wide):
    kv_ref[...] = kv_in[...]
    ig_ref[...] = ig_in[...]
    wide[...] = got_in[...].astype(F32)
    downs, ups = [], []
    for m in range(2):
        pick = jnp.where(iota((512, FN), 0) == idx_ref[m : m + 1, :], 1.0, 0.0).astype(BF)
        down, up = arrived(wide, m)
        downs.append(nt(down, pick))
        ups.append(nt(up, pick))
    gd_ref[...] = downs[0] + downs[1]
    total = ups[0] + ups[1]
    for c in range(4):
        gu_ref[:, c, :] = total[16 * c : 16 * c + 16]


def kernel(
    tok_in, wt_in, cot_in, idx_in, dn_in, up_in,
    kv_ref, ig_ref, got_ref, ids_ref,
    wa, wb, acc, own_kv, rs_send, rs_recv, kvl, igl,
    tok_ref, cot_ref, idx_ref, dn_ref, up_ref, up32, sb32, sb1, sb2, rb32, rb1, rb2, d2t, up2, ar_send, ar_recv,
    wave, s_b8, r_b8, s_loc, s_a, r_a, s_ax, r_ax, s_b, r_b, s_bx, r_bx, s_bf, r_bf,
    s_rs, r_rs, s_ar, r_ar, s_e, r_e, l_e,
):
    z, x = lax.axis_index("z"), lax.axis_index("x")
    tp = lax.axis_index("y") * 2 + lax.axis_index("c")
    f = z * XN + x

    def zmod(v):
        return lax.rem(v + 4 * ZN, ZN)

    def xmod(v):
        return lax.rem(v + 4 * XN, XN)

    def remote(src, dst, send, recv, device):
        return pltpu.make_async_remote_copy(
            src_ref=src, dst_ref=dst, send_sem=send, recv_sem=recv,
            device_id=device, device_id_type=MESH,
        )

    def plane_device(q):
        return {"z": lax.div(q, XN), "x": lax.rem(q, XN)}

    def tp_device(q):
        return {"y": lax.div(q, 2), "c": lax.rem(q, 2)}

    def rows_at(base, size):
        return pl.ds(pl.multiple_of(base, size), size)

    barrier = pltpu.get_barrier_semaphore()
    near = [{"z": zmod(z + 1)}, {"z": zmod(z - 1)}]
    near += [{"x": xmod(x + i)} for i in range(1, XN)]
    near += [tp_device(lax.rem(tp + t, TN)) for t in range(1, TN)]
    for device in near:
        pl.semaphore_signal(barrier, 1, device_id=device, device_id_type=MESH)

    own_rows = rows_at(f * 32, 32)
    loads = [
        pltpu.make_async_copy(src, dst, s_loc.at[n])
        for n, (src, dst) in enumerate(
            (
                (wt_in.at[:, 0:LA], wa.at[own_rows]),
                (wt_in.at[:, LA:1024], wb.at[own_rows]),
                (idx_in, idx_ref),
                (up_in, up_ref),
                (dn_in, dn_ref),
                (tok_in, tok_ref),
                (cot_in, cot_ref),
            )
        )
    ]
    for load in loads:
        load.start()
    loads[0].wait()
    loads[1].wait()
    pl.semaphore_wait(barrier, len(near))

    def wave_on(d, k):
        pl.semaphore_signal(
            wave.at[d, k], 1, device_id=ring_device(d), device_id_type=MESH
        )

    def wave_step(k):
        for d in range(2):
            if k < 8 or d == 0:
                pl.semaphore_wait(wave.at[d, k], 1)
            if k < 7 or (k == 7 and d == 0):
                wave_on(d, k + 1)

    def select(m):
        pick = jnp.where(iota((512, FN), 0) == idx_ref[m : m + 1, :], 1.0, 0.0).astype(BF)
        down = jnp.transpose(nn(dn_ref[...], pick))
        sb32[:, 2 * m, :] = down[:, 0:128]
        sb32[:, 2 * m + 1, :] = down[:, 128:256]
        wide = jnp.concatenate([up32[:, c, :] for c in range(4)], axis=0).astype(BF)
        up = jnp.concatenate([nn(wide, pick), jnp.zeros((64, FN), F32)], axis=0)
        sb32[:, 4 + m, :] = jnp.transpose(up)

    def exchange_start(src, dst, n):
        own = pltpu.make_async_copy(src.at[f], dst.at[f], l_e.at[n])
        own.start()

        @pl.loop(1, FN, unroll=7)
        def _(p):
            q = lax.rem(f + p, FN)
            remote(src.at[q], dst.at[f], s_e.at[n], r_e.at[n], plane_device(q)).start()

    def exchange_wait(src, dst, n):
        pltpu.make_async_copy(src.at[f], dst.at[f], l_e.at[n]).wait()
        remote(
            src.at[0 : FN - 1], dst.at[0 : FN - 1], s_e.at[n], r_e.at[n], plane_device(f)
        ).wait_recv()

    def exchange_drain(src, dst, n):
        remote(
            src.at[0 : FN - 1], dst.at[0 : FN - 1], s_e.at[n], r_e.at[n], plane_device(f)
        ).wait_send()

    def a_rows(d, k, xs):
        zz = zmod(z - k) if d == 0 else zmod(z + k)
        return rows_at(zz * 128 + xs * 32, 32)

    def b_rows(d, k):
        return a_rows(d, k, x)

    def ring_device(d):
        return {"z": zmod(z + 1) if d == 0 else zmod(z - 1)}

    def a_copy(d, k, xs):
        rows = wa.at[a_rows(d, k, xs)]
        return remote(rows, rows, s_a.at[d, k, xs], r_a.at[d, k + 1, xs], ring_device(d))

    def a_wait(d, k, xs):
        rows = wa.at[a_rows(d, k, xs)]
        remote(rows, rows, s_a.at[d, 0, xs], r_a.at[d, k, xs], ring_device(d)).wait_recv()

    def ax_copy(i):
        rows = wa.at[own_rows]
        return remote(rows, rows, s_ax.at[i], r_ax.at[x], {"x": xmod(x + i)})

    def ax_wait(xs):
        rows = wa.at[a_rows(0, 0, xs)]
        remote(rows, rows, s_ax.at[1], r_ax.at[xs], {"x": xmod(x + 1)}).wait_recv()

    def b_copy(d, k):
        rows = wb.at[b_rows(d, k)]
        return remote(rows, rows, s_b.at[d, k], r_b.at[d, k + 1], ring_device(d))

    def b_wait(d, k):
        rows = wb.at[b_rows(d, k)]
        remote(rows, rows, s_b.at[d, 0], r_b.at[d, k], ring_device(d)).wait_recv()

    def b_half(d, k):
        zz = zmod(z - k) if d == 0 else zmod(z + k)
        return wb.at[rows_at(zz * 128 + x * 32 + 16 * d, 16)]

    def b_half_copy(d):
        rows = b_half(d, 7)
        return remote(rows, rows, s_b.at[d, 7], r_b.at[d, 8], ring_device(d))

    def b_half_wait(d):
        rows = b_half(d, 8)
        remote(rows, rows, s_b.at[d, 7], r_b.at[d, 8], ring_device(d)).wait_recv()

    def slot(d, k):
        return k if d == 0 else 8 + k

    def x_device(side):
        return {"x": xmod(x + 1)} if side == 0 else {"x": xmod(x - 1)}

    def bx_rows(d, k, from_x):
        return wb.at[a_rows(d, k, from_x)]

    def bx_copy(side, d, k):
        rows = bx_rows(d, k, x)
        n = slot(d, k)
        return remote(rows, rows, s_bx.at[side, n], r_bx.at[side, n], x_device(side))

    def bx_wait(side, d, k):
        n = slot(d, k)
        rows = bx_rows(d, k, xmod(x - 1) if side == 0 else xmod(x + 1))
        remote(rows, rows, s_bx.at[side, n], r_bx.at[side, n], x_device(side)).wait_recv()

    def bf_rows(side, d, k, from_x):
        zz = zmod(z - k) if d == 0 else zmod(z + k)
        return wb.at[rows_at(zz * 128 + from_x * 32 + 16 * side, 16)]

    def bf_copy(side, d, k):
        n = slot(d, k)
        rows = bf_rows(side, d, k, xmod(x - 1) if side == 0 else xmod(x + 1))
        return remote(rows, rows, s_bf.at[side, n], r_bf.at[side, n], x_device(side))

    def bf_wait(side, d, k):
        n = slot(d, k)
        rows = bf_rows(side, d, k, xmod(x + 2))
        remote(rows, rows, s_bf.at[side, n], r_bf.at[side, n], x_device(side)).wait_recv()

    def b8_copy(d, i):
        rows = b_half(d, 8)
        return remote(rows, rows, s_b8.at[d, i], r_b8.at[d, x], {"x": xmod(x + i)})

    def b8_wait(d, i):
        from_x = xmod(x + i)
        zz = zmod(z + 8)
        rows = wb.at[rows_at(zz * 128 + from_x * 32 + 16 * d, 16)]
        remote(rows, rows, s_b8.at[d, i], r_b8.at[d, from_x], {"x": from_x}).wait_recv()

    def spread(d, k):
        for side in range(2):
            bx_copy(side, d, k).start()

    def forward_x(d, k):
        for side in range(2):
            bx_wait(side, d, k)
            bf_copy(side, d, k).start()

    def complete_x(d, k):
        for side in range(2):
            bf_wait(side, d, k)

    def rs_copy(c):
        return remote(
            rs_send.at[c], rs_recv.at[tp], s_rs.at[c], r_rs.at[tp], tp_device(c)
        )

    def piece(k, j):
        odd = lax.rem(z + k, 2)
        start = zmod(jnp.where(odd == 1, z + k - 1, z - k))
        c = lax.div(start, 2)
        if j < 2:
            rows = rows_at(c * 256 + 128 * j, 128)
            cols = slice(128 * j, 128 * j + 128)
            part = nt(tok_ref[:, 0:LA], wa[rows, :]) + nt(tok_ref[:, LA:1024], wb[rows, :])

            @pl.when(c == tp)
            def _():
                own_kv[:, cols] = part

            @pl.when(c != tp)
            def _():
                rs_send[c, :, cols] = part.astype(BF)
                if j == 1:
                    rs_copy(c).start()

        else:
            rows = rows_at(c * 256, 256)
            cot = cot_ref[:, rows]
            if j == 2:
                acc[:, 0:LA] += nn(cot, wa[rows, :])
                acc[:, LA:512] += nn(cot, wb[rows, 0 : 512 - LA])
            else:
                acc[:, 512:1024] += nn(cot, wb[rows, 512 - LA : LB])

    def block(k):
        for j in range(4):
            piece(k, j)

    rep = jnp.where(lax.div(iota((FN, 1024), 1), 16) == iota((FN, 1024), 0), 1.0, 0.0).astype(BF)
    rep_up = jnp.where(lax.div(iota((FN, 256), 1), 4) == iota((FN, 256), 0), 1.0, 0.0).astype(BF)
    lane16 = lax.rem(iota((16, 1024), 1), 16)
    lane4 = lax.rem(iota((16, 256), 1), 4)
    first = iota((16, 256), 1) < 128
    cot_cols = pl.ds(pl.multiple_of(tp * 256, 256), 256)

    def folded(value):
        return jnp.where(first, value[0:16], value[16:32])

    def unfolded(value):
        return jnp.concatenate(
            [jnp.where(first, value, 0.0), jnp.where(first, 0.0, value)], axis=0
        )

    def adapters():
        exchange_wait(sb1, rb1, 0)
        rb32[...] = rb1[...].astype(F32)
        for m in range(2):
            down, up = arrived(rb32, m)
            wide = nn(down, rep)
            total = jnp.zeros((16, 1024), F32)
            for d in range(16):
                total = jnp.where(lane16 == d, wide[16 * d : 16 * d + 16], total)
            d2t[16 * m : 16 * m + 16] = total.astype(BF)
            wide = nn(up, rep_up)
            total = jnp.zeros((16, 256), F32)
            for d in range(4):
                total = jnp.where(lane4 == d, wide[16 * d : 16 * d + 16], total)
            up2[16 * m : 16 * m + 16] = total.astype(BF)
        ar_send[0:16] = folded(nt(d2t[...], tok_ref[...]))
        ar_send[16:32] = 2.0 * folded(nt(up2[...], cot_ref[:, cot_cols]))
        ar_recv[tp] = ar_send[...]

        @pl.loop(1, TN)
        def _(t):
            ar_copy(t).start()

    def ar_copy(t):
        q = lax.rem(tp + t, TN)
        return remote(ar_send, ar_recv.at[tp], s_ar.at[t], r_ar.at[tp], tp_device(q))

    def tiles():
        @pl.loop(1, TN)
        def _(t):
            q = lax.rem(tp + t, TN)
            remote(ar_send, ar_recv.at[q], s_ar.at[t], r_ar.at[q], tp_device(q)).wait_recv()

        total = ar_recv[0]
        for q in range(1, TN):
            total = total + ar_recv[q]
        low = unfolded(total[0:16].astype(BF).astype(F32))
        back = unfolded(total[16:32].astype(BF).astype(F32))
        low_t, back_t = jnp.transpose(low).astype(BF), jnp.transpose(back).astype(BF)
        low, back = low.astype(BF), back.astype(BF)
        down = nn(back, tok_ref[...])
        up = 2.0 * nn(low, cot_ref[:, cot_cols])
        zeros = jnp.zeros((64, 256), BF)
        for m in range(2):
            mine = down[16 * m : 16 * m + 16]
            wide = jnp.concatenate(
                [jnp.where(lane16 == d, mine, 0.0).astype(BF) for d in range(16)], axis=0
            )
            packed = jnp.transpose(nt(wide, rep))
            sb32[:, 2 * m, :] = packed[:, 0:128]
            sb32[:, 2 * m + 1, :] = packed[:, 128:256]
            mine = up[16 * m : 16 * m + 16]
            wide = jnp.concatenate(
                [jnp.where(lane4 == d, mine, 0.0).astype(BF) for d in range(4)] + [zeros], axis=0
            )
            sb32[:, 4 + m, :] = jnp.transpose(nt(wide, rep_up))
        sb2[...] = sb32[...].astype(BF)
        exchange_start(sb2, rb2, 1)
        kvl[...] = (2.0 * nn(low_t, up2[...])).astype(BF)
        igl[...] = nn(back_t, d2t[...]).astype(BF)

    for i in range(1, XN):
        ax_copy(i).start()
    for d in range(2):
        b_copy(d, 0).start()
        a_copy(d, 0, x).start()
        wave_on(d, 1)
    spread(0, 0)
    for load in loads[2:5]:
        load.wait()
    up32[...] = up_ref[...].astype(F32)
    sb32[...] = jnp.zeros_like(sb32)

    def ring_b(k):
        for d in range(2):
            b_wait(d, k)

            @pl.when(k < 7)
            def _():
                b_copy(d, k).start()

            @pl.when(k == 7)
            def _():
                b_half_copy(d).start()

            spread(d, k)

    def ring_a(k, i):
        xs = xmod(x + i)
        for d in range(2):
            a_wait(d, k, xs)

            @pl.when((k < 7) | (lax.div(xs, 2) == d))
            def _():
                a_copy(d, k, xs).start()

    wave_step(1)
    select(0)
    wave_step(2)
    for i in range(1, XN):
        xs = xmod(x + i)
        ax_wait(xs)
        for d in range(2):
            a_copy(d, 0, xs).start()
    select(1)
    wave_step(3)
    sb1[...] = sb32[...].astype(BF)
    ring_b(1)
    wave_step(4)
    for i in range(XN):
        ring_a(1, i)
    wave_step(5)
    forward_x(0, 0)
    for k in range(6, 9):
        wave_step(k)
    exchange_start(sb1, rb1, 0)
    acc[...] = jnp.zeros_like(acc)
    loads[5].wait()
    loads[6].wait()

    @pl.loop(2, 8)
    def _(k):
        ring_b(k)
        for i in range(XN):
            ring_a(k, i)

            @pl.when(k >= 4)
            def _():
                piece(k - 3, i)

        for d in range(2):
            forward_x(d, k - 1)

        @pl.when(k == 2)
        def _():
            complete_x(0, 0)

        @pl.when(k >= 3)
        def _():
            for d in range(2):
                complete_x(d, k - 2)

        @pl.when(k == ADAPT_AT)
        def _():
            adapters()

        @pl.when(k == TILES_AT)
        def _():
            tiles()

    for d in range(2):
        b_half_wait(d)
        for i in range(1, XN):
            b8_copy(d, i).start()
    for h in range(2):
        for d in range(2):
            a_wait(d, 8, 2 * d + h)
        piece(5, h)
    for d in range(2):
        forward_x(d, 7)
    piece(5, 2)
    piece(5, 3)
    for d in range(2):
        complete_x(d, 6)
    block(6)
    for d in range(2):
        complete_x(d, 7)
    block(7)
    for d in range(2):
        for i in range(1, XN):
            b8_wait(d, i)
    block(8)
    ig_ref[...] = (acc[...] + igl[...].astype(F32)).astype(BF)
    exchange_wait(sb2, rb2, 1)
    got_ref[...] = rb2[...]
    ids_ref[...] = idx_ref[...]

    total = own_kv[...]
    for t in range(1, TN):
        q = lax.rem(tp + t, TN)
        remote(
            rs_send.at[q], rs_recv.at[q], s_rs.at[q], r_rs.at[q], tp_device(q)
        ).wait_recv()
        total = total + rs_recv[q].astype(F32)
    kv_ref[...] = (total + kvl[...].astype(F32)).astype(BF)

    exchange_drain(sb1, rb1, 0)
    exchange_drain(sb2, rb2, 1)
    for i in range(1, XN):
        ax_copy(i).wait_send()

    @pl.loop(1, TN)
    def _(t):
        ar_copy(t).wait_send()
        rs_copy(lax.rem(tp + t, TN)).wait_send()

    for d in range(2):

        @pl.loop(0, 7)
        def _(k):
            for xs in range(XN):
                a_copy(d, k, xs).wait_send()
            b_copy(d, k).wait_send()

        for h in range(2):
            a_copy(d, 7, 2 * d + h).wait_send()
        b_half_copy(d).wait_send()
    for d in range(2):
        for i in range(1, XN):
            b8_copy(d, i).wait_send()
    for side in range(2):

        @pl.loop(0, 8)
        def _(k):
            bx_copy(side, 0, k).wait_send()
            bf_copy(side, 0, k).wait_send()

        @pl.loop(1, 8)
        def _(k):
            bx_copy(side, 1, k).wait_send()
            bf_copy(side, 1, k).wait_send()


def fused(tok, wt, cot, idx, dn, up):
    dma = pltpu.SemaphoreType.DMA
    vmem = pl.BlockSpec(memory_space=pltpu.VMEM)
    kv, ig, got, ids = pl.pallas_call(
        kernel,
        out_shape=(
            jax.ShapeDtypeStruct((256, 256), BF),
            jax.ShapeDtypeStruct((256, 1024), BF),
            jax.ShapeDtypeStruct((FN, 8, 128), BF),
            jax.ShapeDtypeStruct((2, FN), jnp.int32),
        ),
        in_specs=[pl.BlockSpec(memory_space=pltpu.HBM)] * 6,
        out_specs=[vmem] * 4,
        scratch_shapes=[
            pltpu.VMEM((2048, LA), BF),
            pltpu.VMEM((2048, LB), BF),
            pltpu.VMEM((256, 1024), F32),
            pltpu.VMEM((256, 256), F32),
            pltpu.VMEM((TN, 256, 256), BF),
            pltpu.VMEM((TN, 256, 256), BF),
            pltpu.VMEM((256, 256), BF),
            pltpu.VMEM((256, 1024), BF),
            pltpu.VMEM((256, 1024), BF),
            pltpu.VMEM((256, 2048), BF),
            pltpu.VMEM((2, FN), jnp.int32),
            pltpu.VMEM((256, 512), BF),
            pltpu.VMEM((16, 4, 512), BF),
            pltpu.VMEM((16, 4, 512), F32),
            pltpu.VMEM((FN, 8, 128), F32),
            pltpu.VMEM((FN, 8, 128), BF),
            pltpu.VMEM((FN, 8, 128), BF),
            pltpu.VMEM((FN, 8, 128), F32),
            pltpu.VMEM((FN, 8, 128), BF),
            pltpu.VMEM((FN, 8, 128), BF),
            pltpu.VMEM((32, 1024), BF),
            pltpu.VMEM((32, 256), BF),
            pltpu.VMEM((32, 256), F32),
            pltpu.VMEM((TN, 32, 256), F32),
            pltpu.SemaphoreType.REGULAR((2, 9)),
            dma((2, XN)),
            dma((2, XN)),
            dma((7,)),
            dma((2, 8, XN)),
            dma((2, 9, XN)),
            dma((XN,)),
            dma((XN,)),
            dma((2, 8)),
            dma((2, 9)),
            dma((2, 16)),
            dma((2, 16)),
            dma((2, 16)),
            dma((2, 16)),
            dma((TN,)),
            dma((TN,)),
            dma((TN,)),
            dma((TN,)),
            dma((2,)),
            dma((2,)),
            dma((2,)),
        ],
        compiler_params=pltpu.CompilerParams(
            collective_id=0, has_side_effects=True, vmem_limit_bytes=32 << 20
        ),
    )(*(pltpu.with_memory_space_constraint(v, pltpu.HBM) for v in (tok, wt, cot, idx, dn, up)))
    return pl.pallas_call(
        finish,
        out_shape=(
            jax.ShapeDtypeStruct((256, 256), BF),
            jax.ShapeDtypeStruct((256, 1024), BF),
            jax.ShapeDtypeStruct((256, 512), F32),
            jax.ShapeDtypeStruct((16, 4, 512), F32),
        ),
        in_specs=[vmem] * 4,
        out_specs=[vmem] * 4,
        scratch_shapes=[pltpu.VMEM((FN, 8, 128), F32)],
        compiler_params=pltpu.CompilerParams(vmem_limit_bytes=16 << 20),
    )(kv, ig, got, ids)


def local(tokens, frozen_weight, cotangent, block_adapter_index, down_weight, up_weight):
    tok = tokens.reshape(256, 1024)
    cot = cotangent.reshape(256, 2048)
    wt = frozen_weight.T
    dn = down_weight.transpose(1, 2, 0).reshape(256, 512)
    up = up_weight.transpose(1, 2, 0)
    kv, ig, gd, gu = fused(tok, wt, cot, block_adapter_index, dn, up)
    return (
        kv.reshape(2, 128, 256),
        ig.reshape(2, 128, 1024),
        gd.reshape(16, 16, 512).transpose(2, 0, 1),
        gu.transpose(2, 0, 1),
    )


def solution(mesh):
    finer = Mesh(mesh.devices.reshape(ZN, XN, 4, 2), ("z", "x", "y", "c"))
    return jax.shard_map(
        local,
        mesh=finer,
        in_specs=(
            P(None, PLANE, TP),
            P(TP, PLANE),
            P(None, PLANE, None),
            P(),
            P(None, ALL, None),
            P(None, None, ALL),
        ),
        out_specs=(
            P(None, PLANE, TP),
            P(None, PLANE, TP),
            P(None, ALL, None),
            P(None, None, ALL),
        ),
        check_vma=False,
    )
```

```python
import functools

import jax
import jax.numpy as jnp
from jax import lax
from jax.experimental import pallas as pl
from jax.experimental.pallas import tpu as pltpu
from jax.sharding import Mesh
from jax.sharding import PartitionSpec as P

MESH = pl.DeviceIdType.MESH
PLANE = ("z", "x")
TP = ("y", "c")
ALL = ("y", "c", "z", "x")

ZN, XN, TN = 16, 4, 8
FN = ZN * XN
BF = jnp.bfloat16
F32 = jnp.float32
NA = 2
LA = NA * 128
LB = 1024 - LA
ADAPT_AT = 5
TILES_AT = 7


def nt(a, b):
    return lax.dot_general(a, b, (((1,), (1,)), ((), ())), preferred_element_type=F32)


def nn(a, b):
    return jnp.dot(a, b, preferred_element_type=F32)


def iota(shape, dim):
    return lax.broadcasted_iota(jnp.int32, shape, dim)


def arrived(ref, m):
    down = [jnp.transpose(ref[:, 2 * m + h, :]) for h in range(2)]
    up = jnp.transpose(ref[:, 4 + m, :])[0:64, :]
    return jnp.concatenate(down, axis=0).astype(BF), up.astype(BF)


def finish(kv_in, ig_in, got_in, idx_ref, kv_ref, ig_ref, gd_ref, gu_ref, wide):
    kv_ref[...] = kv_in[...]
    ig_ref[...] = ig_in[...]
    wide[...] = got_in[...].astype(F32)
    downs, ups = [], []
    for m in range(2):
        pick = jnp.where(iota((512, FN), 0) == idx_ref[m : m + 1, :], 1.0, 0.0).astype(BF)
        down, up = arrived(wide, m)
        downs.append(nt(down, pick))
        ups.append(nt(up, pick))
    gd_ref[...] = downs[0] + downs[1]
    total = ups[0] + ups[1]
    for c in range(4):
        gu_ref[:, c, :] = total[16 * c : 16 * c + 16]


def kernel(
    tok_in, wt_in, cot_in, idx_in, dn_in, up_in,
    kv_ref, ig_ref, got_ref, ids_ref,
    wa, wb, acc, own_kv, rs_send, rs_recv, low_t, back_t,
    tok_ref, cot_ref, idx_ref, dn_ref, up_ref, up32, sb32, sb1, sb2, rb32, rb1, rb2, d2t, up2, ar_send, ar_recv,
    wave, s_b8, r_b8, s_loc, s_a, r_a, s_ax, r_ax, s_b, r_b, s_bx, r_bx, s_bf, r_bf,
    s_rs, r_rs, s_ar, r_ar, s_e, r_e, l_e,
):
    z, x = lax.axis_index("z"), lax.axis_index("x")
    tp = lax.axis_index("y") * 2 + lax.axis_index("c")
    f = z * XN + x

    def zmod(v):
        return lax.rem(v + 4 * ZN, ZN)

    def xmod(v):
        return lax.rem(v + 4 * XN, XN)

    def remote(src, dst, send, recv, device):
        return pltpu.make_async_remote_copy(
            src_ref=src, dst_ref=dst, send_sem=send, recv_sem=recv,
            device_id=device, device_id_type=MESH,
        )

    def plane_device(q):
        return {"z": lax.div(q, XN), "x": lax.rem(q, XN)}

    def tp_device(q):
        return {"y": lax.div(q, 2), "c": lax.rem(q, 2)}

    def rows_at(base, size):
        return pl.ds(pl.multiple_of(base, size), size)

    barrier = pltpu.get_barrier_semaphore()
    near = [{"z": zmod(z + 1)}, {"z": zmod(z - 1)}]
    near += [{"x": xmod(x + i)} for i in range(1, XN)]
    near += [tp_device(lax.rem(tp + t, TN)) for t in range(1, TN)]
    for device in near:
        pl.semaphore_signal(barrier, 1, device_id=device, device_id_type=MESH)

    own_rows = rows_at(f * 32, 32)
    loads = [
        pltpu.make_async_copy(src, dst, s_loc.at[n])
        for n, (src, dst) in enumerate(
            (
                (wt_in.at[:, 0:LA], wa.at[own_rows]),
                (wt_in.at[:, LA:1024], wb.at[own_rows]),
                (idx_in, idx_ref),
                (up_in, up_ref),
                (dn_in, dn_ref),
                (tok_in, tok_ref),
                (cot_in, cot_ref),
            )
        )
    ]
    for load in loads:
        load.start()
    loads[0].wait()
    loads[1].wait()
    pl.semaphore_wait(barrier, len(near))

    def wave_on(d, k):
        pl.semaphore_signal(
            wave.at[d, k], 1, device_id=ring_device(d), device_id_type=MESH
        )

    def wave_step(k):
        for d in range(2):
            if k < 8 or d == 0:
                pl.semaphore_wait(wave.at[d, k], 1)
            if k < 7 or (k == 7 and d == 0):
                wave_on(d, k + 1)

    def select(m):
        pick = jnp.where(iota((512, FN), 0) == idx_ref[m : m + 1, :], 1.0, 0.0).astype(BF)
        down = jnp.transpose(nn(dn_ref[...], pick))
        sb32[:, 2 * m, :] = down[:, 0:128]
        sb32[:, 2 * m + 1, :] = down[:, 128:256]
        wide = jnp.concatenate([up32[:, c, :] for c in range(4)], axis=0).astype(BF)
        up = jnp.concatenate([nn(wide, pick), jnp.zeros((64, FN), F32)], axis=0)
        sb32[:, 4 + m, :] = jnp.transpose(up)

    def exchange_start(src, dst, n):
        own = pltpu.make_async_copy(src.at[f], dst.at[f], l_e.at[n])
        own.start()

        @pl.loop(1, FN, unroll=7)
        def _(p):
            q = lax.rem(f + p, FN)
            remote(src.at[q], dst.at[f], s_e.at[n], r_e.at[n], plane_device(q)).start()

    def exchange_wait(src, dst, n):
        pltpu.make_async_copy(src.at[f], dst.at[f], l_e.at[n]).wait()
        remote(
            src.at[0 : FN - 1], dst.at[0 : FN - 1], s_e.at[n], r_e.at[n], plane_device(f)
        ).wait_recv()

    def exchange_drain(src, dst, n):
        remote(
            src.at[0 : FN - 1], dst.at[0 : FN - 1], s_e.at[n], r_e.at[n], plane_device(f)
        ).wait_send()

    def a_rows(d, k, xs):
        zz = zmod(z - k) if d == 0 else zmod(z + k)
        return rows_at(zz * 128 + xs * 32, 32)

    def b_rows(d, k):
        return a_rows(d, k, x)

    def ring_device(d):
        return {"z": zmod(z + 1) if d == 0 else zmod(z - 1)}

    def a_copy(d, k, xs):
        rows = wa.at[a_rows(d, k, xs)]
        return remote(rows, rows, s_a.at[d], r_a.at[d, k + 1, xs], ring_device(d))

    def a_wait(d, k, xs):
        rows = wa.at[a_rows(d, k, xs)]
        remote(rows, rows, s_a.at[d], r_a.at[d, k, xs], ring_device(d)).wait_recv()

    def ax_copy(i):
        rows = wa.at[own_rows]
        return remote(rows, rows, s_ax, r_ax.at[x], {"x": xmod(x + i)})

    def ax_wait(xs):
        rows = wa.at[a_rows(0, 0, xs)]
        remote(rows, rows, s_ax, r_ax.at[xs], {"x": xmod(x + 1)}).wait_recv()

    def b_copy(d, k):
        rows = wb.at[b_rows(d, k)]
        return remote(rows, rows, s_b.at[d], r_b.at[d, k + 1], ring_device(d))

    def b_wait(d, k):
        rows = wb.at[b_rows(d, k)]
        remote(rows, rows, s_b.at[d], r_b.at[d, k], ring_device(d)).wait_recv()

    def b_half(d, k):
        zz = zmod(z - k) if d == 0 else zmod(z + k)
        return wb.at[rows_at(zz * 128 + x * 32 + 16 * d, 16)]

    def b_half_copy(d):
        rows = b_half(d, 7)
        return remote(rows, rows, s_b.at[d], r_b.at[d, 8], ring_device(d))

    def b_half_wait(d):
        rows = b_half(d, 8)
        remote(rows, rows, s_b.at[d], r_b.at[d, 8], ring_device(d)).wait_recv()

    def slot(d, k):
        return k if d == 0 else 8 + k

    def x_device(side):
        return {"x": xmod(x + 1)} if side == 0 else {"x": xmod(x - 1)}

    def bx_rows(d, k, from_x):
        return wb.at[a_rows(d, k, from_x)]

    def bx_copy(side, d, k):
        rows = bx_rows(d, k, x)
        n = slot(d, k)
        return remote(rows, rows, s_bx.at[side], r_bx.at[side, n], x_device(side))

    def bx_wait(side, d, k):
        n = slot(d, k)
        rows = bx_rows(d, k, xmod(x - 1) if side == 0 else xmod(x + 1))
        remote(rows, rows, s_bx.at[side], r_bx.at[side, n], x_device(side)).wait_recv()

    def bf_rows(side, d, k, from_x):
        zz = zmod(z - k) if d == 0 else zmod(z + k)
        return wb.at[rows_at(zz * 128 + from_x * 32 + 16 * side, 16)]

    def bf_copy(side, d, k):
        n = slot(d, k)
        rows = bf_rows(side, d, k, xmod(x - 1) if side == 0 else xmod(x + 1))
        return remote(rows, rows, s_bf.at[side], r_bf.at[side, n], x_device(side))

    def bf_wait(side, d, k):
        n = slot(d, k)
        rows = bf_rows(side, d, k, xmod(x + 2))
        remote(rows, rows, s_bf.at[side], r_bf.at[side, n], x_device(side)).wait_recv()

    def b8_copy(d, i):
        rows = b_half(d, 8)
        return remote(rows, rows, s_b8, r_b8.at[d, x], {"x": xmod(x + i)})

    def b8_wait(d, i):
        from_x = xmod(x + i)
        zz = zmod(z + 8)
        rows = wb.at[rows_at(zz * 128 + from_x * 32 + 16 * d, 16)]
        remote(rows, rows, s_b8, r_b8.at[d, from_x], {"x": from_x}).wait_recv()

    def spread(d, k):
        for side in range(2):
            bx_copy(side, d, k).start()

    def forward_x(d, k):
        for side in range(2):
            bx_wait(side, d, k)
            bf_copy(side, d, k).start()

    def complete_x(d, k):
        for side in range(2):
            bf_wait(side, d, k)

    def rs_copy(zz):
        c, h = lax.div(zz, 2), lax.rem(zz, 2)
        return remote(
            rs_send.at[zz], rs_recv.at[tp, h], s_rs, r_rs.at[tp, h], tp_device(c)
        )

    def kv_piece(d, k):
        zz = zmod(z - k) if d == 0 else zmod(z + k)
        c = lax.div(zz, 2)
        rows = rows_at(zz * 128, 128)
        part = nt(tok_ref[:, 0:LA], wa[rows, :]) + nt(tok_ref[:, LA:1024], wb[rows, :])

        @pl.when(c == tp)
        def _():
            own_kv[lax.rem(zz, 2)] = part

        @pl.when(c != tp)
        def _():
            rs_send[zz] = part.astype(BF)
            rs_copy(zz).start()

    def ig_piece(k, j):
        odd = lax.rem(z + k, 2)
        start = zmod(jnp.where(odd == 1, z + k - 1, z - k))
        rows = rows_at(start * 128, 256)
        cot = cot_ref[:, rows]
        if j == 0:
            acc[:, 0:LA] += nn(cot, wa[rows, :])
            acc[:, LA:512] += nn(cot, wb[rows, 0 : 512 - LA])
        else:
            acc[:, 512:1024] += nn(cot, wb[rows, 512 - LA : LB])

    def piece(k, j):
        if j < 2:
            kv_piece(j, k)
        else:
            ig_piece(k, j - 2)

    def block(k):
        for j in range(4):
            piece(k, j)

    rep = jnp.where(lax.div(iota((FN, 1024), 1), 16) == iota((FN, 1024), 0), 1.0, 0.0).astype(BF)
    rep_up = jnp.where(lax.div(iota((FN, 256), 1), 4) == iota((FN, 256), 0), 1.0, 0.0).astype(BF)
    lane16 = lax.rem(iota((16, 1024), 1), 16)
    lane4 = lax.rem(iota((16, 256), 1), 4)
    first = iota((16, 256), 1) < 128
    cot_cols = pl.ds(pl.multiple_of(tp * 256, 256), 256)

    def folded(value):
        return jnp.where(first, value[0:16], value[16:32])

    def unfolded(value):
        return jnp.concatenate(
            [jnp.where(first, value, 0.0), jnp.where(first, 0.0, value)], axis=0
        )

    def adapters():
        exchange_wait(sb1, rb1, 0)
        rb32[...] = rb1[...].astype(F32)
        for m in range(2):
            down, up = arrived(rb32, m)
            wide = nn(down, rep)
            total = jnp.zeros((16, 1024), F32)
            for d in range(16):
                total = jnp.where(lane16 == d, wide[16 * d : 16 * d + 16], total)
            d2t[16 * m : 16 * m + 16] = total.astype(BF)
            wide = nn(up, rep_up)
            total = jnp.zeros((16, 256), F32)
            for d in range(4):
                total = jnp.where(lane4 == d, wide[16 * d : 16 * d + 16], total)
            up2[16 * m : 16 * m + 16] = total.astype(BF)
        ar_send[0:16] = folded(nt(d2t[...], tok_ref[...]))
        ar_send[16:32] = 2.0 * folded(nt(up2[...], cot_ref[:, cot_cols]))
        ar_recv[tp] = ar_send[...]

        @pl.loop(1, TN)
        def _(t):
            ar_copy(t).start()

    def ar_copy(t):
        q = lax.rem(tp + t, TN)
        return remote(ar_send, ar_recv.at[tp], s_ar, r_ar.at[tp], tp_device(q))

    def tiles():
        @pl.loop(1, TN)
        def _(t):
            q = lax.rem(tp + t, TN)
            remote(ar_send, ar_recv.at[q], s_ar, r_ar.at[q], tp_device(q)).wait_recv()

        total = ar_recv[0]
        for q in range(1, TN):
            total = total + ar_recv[q]
        low = unfolded(total[0:16].astype(BF).astype(F32))
        back = unfolded(total[16:32].astype(BF).astype(F32))
        low_t[...] = jnp.transpose(low).astype(BF)
        back_t[...] = jnp.transpose(back).astype(BF)
        low, back = low.astype(BF), back.astype(BF)
        down = nn(back, tok_ref[...])
        up = 2.0 * nn(low, cot_ref[:, cot_cols])
        zeros = jnp.zeros((64, 256), BF)
        for m in range(2):
            mine = down[16 * m : 16 * m + 16]
            wide = jnp.concatenate(
                [jnp.where(lane16 == d, mine, 0.0).astype(BF) for d in range(16)], axis=0
            )
            packed = jnp.transpose(nt(wide, rep))
            sb32[:, 2 * m, :] = packed[:, 0:128]
            sb32[:, 2 * m + 1, :] = packed[:, 128:256]
            mine = up[16 * m : 16 * m + 16]
            wide = jnp.concatenate(
                [jnp.where(lane4 == d, mine, 0.0).astype(BF) for d in range(4)] + [zeros], axis=0
            )
            sb32[:, 4 + m, :] = jnp.transpose(nt(wide, rep_up))
        sb2[...] = sb32[...].astype(BF)
        exchange_start(sb2, rb2, 1)

    for i in range(1, XN):
        ax_copy(i).start()
    for d in range(2):
        b_copy(d, 0).start()
        a_copy(d, 0, x).start()
        wave_on(d, 1)
    spread(0, 0)
    for load in loads[2:5]:
        load.wait()
    up32[...] = up_ref[...].astype(F32)
    sb32[...] = jnp.zeros_like(sb32)

    def ring_b(k):
        for d in range(2):
            b_wait(d, k)

            @pl.when(k < 7)
            def _():
                b_copy(d, k).start()

            @pl.when(k == 7)
            def _():
                b_half_copy(d).start()

            spread(d, k)

    def ring_a(k, i):
        xs = xmod(x + i)
        for d in range(2):
            a_wait(d, k, xs)

            @pl.when((k < 7) | (lax.div(xs, 2) == d))
            def _():
                a_copy(d, k, xs).start()

    wave_step(1)
    select(0)
    wave_step(2)
    for i in range(1, XN):
        xs = xmod(x + i)
        ax_wait(xs)
        for d in range(2):
            a_copy(d, 0, xs).start()
    select(1)
    wave_step(3)
    sb1[...] = sb32[...].astype(BF)
    ring_b(1)
    wave_step(4)
    for i in range(XN):
        ring_a(1, i)
    wave_step(5)
    forward_x(0, 0)
    ring_b(2)
    wave_step(6)
    for i in range(XN):
        ring_a(2, i)
    for d in range(2):
        forward_x(d, 1)
    complete_x(0, 0)
    wave_step(7)
    wave_step(8)
    exchange_start(sb1, rb1, 0)
    acc[...] = jnp.zeros_like(acc)
    loads[5].wait()
    loads[6].wait()

    @pl.loop(3, 8)
    def _(k):
        ring_b(k)
        for i in range(XN):
            ring_a(k, i)

            if i == 0:
                piece(k - 3, i)
            else:

                @pl.when(k >= 4)
                def _():
                    piece(k - 3, i)

        for d in range(2):
            forward_x(d, k - 1)
        for d in range(2):
            complete_x(d, k - 2)

        @pl.when(k == ADAPT_AT)
        def _():
            adapters()

        @pl.when(k == TILES_AT)
        def _():
            tiles()

    piece(5, 0)
    piece(5, 1)
    for d in range(2):
        forward_x(d, 7)
    for d in range(2):
        b_half_wait(d)
        for i in range(1, XN):
            b8_copy(d, i).start()
    for h in range(2):
        for d in range(2):
            a_wait(d, 8, 2 * d + h)
    piece(5, 2)
    piece(5, 3)
    for d in range(2):
        complete_x(d, 6)
    block(6)
    for d in range(2):
        complete_x(d, 7)
    kv_piece(0, 7)
    kv_piece(1, 7)
    for d in range(2):
        for i in range(1, XN):
            b8_wait(d, i)
    kv_piece(0, 8)
    for k in (7, 8):
        for j in range(2):
            ig_piece(k, j)
    ig_ref[...] = (acc[...] + nn(back_t[...], d2t[...]).astype(BF).astype(F32)).astype(BF)
    kvl = (2.0 * nn(low_t[...], up2[...])).astype(BF).astype(F32)
    exchange_wait(sb2, rb2, 1)
    got_ref[...] = rb2[...]
    ids_ref[...] = idx_ref[...]

    for h in range(2):
        cols = slice(128 * h, 128 * h + 128)
        total = own_kv[h]
        for t in range(1, TN):
            q = lax.rem(tp + t, TN)
            remote(
                rs_send.at[0], rs_recv.at[q, h], s_rs, r_rs.at[q, h], tp_device(q)
            ).wait_recv()
            total = total + rs_recv[q, h].astype(F32)
        kv_ref[:, cols] = (total + kvl[:, cols]).astype(BF)

    def drain(ref, sem):
        remote(ref, ref, sem, s_loc.at[0], ring_device(0)).wait_send()

    exchange_drain(sb1, rb1, 0)
    exchange_drain(sb2, rb2, 1)
    drain(wa.at[0:96], s_ax)
    drain(wb.at[0:96], s_b8)
    drain(ar_recv.at[0 : TN - 1], s_ar)
    drain(rs_send.at[0 : 2 * TN - 2], s_rs)
    for d in range(2):
        drain(wa.at[0:960], s_a.at[d])
        drain(wb.at[0:240], s_b.at[d])
        drain(wb.at[0:480], s_bx.at[d])
        drain(wb.at[0:240], s_bf.at[d])


def fused(tok, wt, cot, idx, dn, up):
    dma = pltpu.SemaphoreType.DMA
    vmem = pl.BlockSpec(memory_space=pltpu.VMEM)
    kv, ig, got, ids = pl.pallas_call(
        kernel,
        out_shape=(
            jax.ShapeDtypeStruct((256, 256), BF),
            jax.ShapeDtypeStruct((256, 1024), BF),
            jax.ShapeDtypeStruct((FN, 8, 128), BF),
            jax.ShapeDtypeStruct((2, FN), jnp.int32),
        ),
        in_specs=[pl.BlockSpec(memory_space=pltpu.HBM)] * 6,
        out_specs=[vmem] * 4,
        scratch_shapes=[
            pltpu.VMEM((2048, LA), BF),
            pltpu.VMEM((2048, LB), BF),
            pltpu.VMEM((256, 1024), F32),
            pltpu.VMEM((2, 256, 128), F32),
            pltpu.VMEM((ZN, 256, 128), BF),
            pltpu.VMEM((TN, 2, 256, 128), BF),
            pltpu.VMEM((256, 32), BF),
            pltpu.VMEM((256, 32), BF),
            pltpu.VMEM((256, 1024), BF),
            pltpu.VMEM((256, 2048), BF),
            pltpu.VMEM((2, FN), jnp.int32),
            pltpu.VMEM((256, 512), BF),
            pltpu.VMEM((16, 4, 512), BF),
            pltpu.VMEM((16, 4, 512), F32),
            pltpu.VMEM((FN, 8, 128), F32),
            pltpu.VMEM((FN, 8, 128), BF),
            pltpu.VMEM((FN, 8, 128), BF),
            pltpu.VMEM((FN, 8, 128), F32),
            pltpu.VMEM((FN, 8, 128), BF),
            pltpu.VMEM((FN, 8, 128), BF),
            pltpu.VMEM((32, 1024), BF),
            pltpu.VMEM((32, 256), BF),
            pltpu.VMEM((32, 256), F32),
            pltpu.VMEM((TN, 32, 256), F32),
            pltpu.SemaphoreType.REGULAR((2, 9)),
            dma(()),
            dma((2, XN)),
            dma((7,)),
            dma((2,)),
            dma((2, 9, XN)),
            dma(()),
            dma((XN,)),
            dma((2,)),
            dma((2, 9)),
            dma((2,)),
            dma((2, 16)),
            dma((2,)),
            dma((2, 16)),
            dma(()),
            dma((TN, 2)),
            dma(()),
            dma((TN,)),
            dma((2,)),
            dma((2,)),
            dma((2,)),
        ],
        compiler_params=pltpu.CompilerParams(
            collective_id=0, has_side_effects=True, vmem_limit_bytes=32 << 20
        ),
    )(*(pltpu.with_memory_space_constraint(v, pltpu.HBM) for v in (tok, wt, cot, idx, dn, up)))
    return pl.pallas_call(
        finish,
        out_shape=(
            jax.ShapeDtypeStruct((256, 256), BF),
            jax.ShapeDtypeStruct((256, 1024), BF),
            jax.ShapeDtypeStruct((256, 512), F32),
            jax.ShapeDtypeStruct((16, 4, 512), F32),
        ),
        in_specs=[vmem] * 4,
        out_specs=[vmem] * 4,
        scratch_shapes=[pltpu.VMEM((FN, 8, 128), F32)],
        compiler_params=pltpu.CompilerParams(vmem_limit_bytes=16 << 20),
    )(kv, ig, got, ids)


def local(tokens, frozen_weight, cotangent, block_adapter_index, down_weight, up_weight):
    tok = tokens.reshape(256, 1024)
    cot = cotangent.reshape(256, 2048)
    wt = frozen_weight.T
    dn = down_weight.transpose(1, 2, 0).reshape(256, 512)
    up = up_weight.transpose(1, 2, 0)
    kv, ig, gd, gu = fused(tok, wt, cot, block_adapter_index, dn, up)
    return (
        kv.reshape(2, 128, 256),
        ig.reshape(2, 128, 1024),
        gd.reshape(16, 16, 512).transpose(2, 0, 1),
        gu.transpose(2, 0, 1),
    )


def solution(mesh):
    finer = Mesh(mesh.devices.reshape(ZN, XN, 4, 2), ("z", "x", "y", "c"))
    return jax.shard_map(
        local,
        mesh=finer,
        in_specs=(
            P(None, PLANE, TP),
            P(TP, PLANE),
            P(None, PLANE, None),
            P(),
            P(None, ALL, None),
            P(None, None, ALL),
        ),
        out_specs=(
            P(None, PLANE, TP),
            P(None, PLANE, TP),
            P(None, ALL, None),
            P(None, None, ALL),
        ),
        check_vma=False,
    )
```

```python
import functools

import jax
import jax.numpy as jnp
from jax import lax
from jax.experimental import pallas as pl
from jax.experimental.pallas import tpu as pltpu
from jax.sharding import Mesh
from jax.sharding import PartitionSpec as P

MESH = pl.DeviceIdType.MESH
PLANE = ("z", "x")
TP = ("y", "c")
ALL = ("y", "c", "z", "x")

ZN, XN, TN = 16, 4, 8
FN = ZN * XN
BF = jnp.bfloat16
F32 = jnp.float32
NA = 2
LA = NA * 128
LB = 1024 - LA
ADAPT_AT = 5
TILES_AT = 7


def nt(a, b):
    return lax.dot_general(a, b, (((1,), (1,)), ((), ())), preferred_element_type=F32)


def nn(a, b):
    return jnp.dot(a, b, preferred_element_type=F32)


def iota(shape, dim):
    return lax.broadcasted_iota(jnp.int32, shape, dim)


def arrived(ref, m):
    down = [jnp.transpose(ref[:, 2 * m + h, :]) for h in range(2)]
    up = jnp.transpose(ref[:, 4 + m, :])[0:64, :]
    return jnp.concatenate(down, axis=0).astype(BF), up.astype(BF)


def finish(kv_in, ig_in, got_in, idx_ref, kv_ref, ig_ref, gd_ref, gu_ref, wide):
    kv_ref[...] = kv_in[...]
    ig_ref[...] = ig_in[...]
    wide[...] = got_in[...].astype(F32)
    downs, ups = [], []
    for m in range(2):
        pick = jnp.where(iota((512, FN), 0) == idx_ref[m : m + 1, :], 1.0, 0.0).astype(BF)
        down, up = arrived(wide, m)
        downs.append(nt(down, pick))
        ups.append(nt(up, pick))
    gd_ref[...] = downs[0] + downs[1]
    total = ups[0] + ups[1]
    for c in range(4):
        gu_ref[:, c, :] = total[16 * c : 16 * c + 16]


def kernel(
    tok_in, wt_in, cot_in, idx_in, dn_in, up_in,
    kv_ref, ig_ref, got_ref, ids_ref,
    wa, wb, acc, own_kv, rs_send, rs_recv, low_t, back_t,
    tok_ref, cot_ref, idx_ref, dn_ref, up_ref, up32, sb32, sb1, sb2, rb32, rb1, rb2, d2t, up2, ar_send, ar_recv,
    wave, s_b8, r_b8, s_loc, s_a, r_a, s_ax, r_ax, s_b, r_b, s_bx, r_bx, s_bf, r_bf,
    s_rs, r_rs, s_ar, r_ar, s_e, r_e, l_e,
):
    z, x = lax.axis_index("z"), lax.axis_index("x")
    tp = lax.axis_index("y") * 2 + lax.axis_index("c")
    f = z * XN + x

    def zmod(v):
        return lax.rem(v + 4 * ZN, ZN)

    def xmod(v):
        return lax.rem(v + 4 * XN, XN)

    def remote(src, dst, send, recv, device):
        return pltpu.make_async_remote_copy(
            src_ref=src, dst_ref=dst, send_sem=send, recv_sem=recv,
            device_id=device, device_id_type=MESH,
        )

    def plane_device(q):
        return {"z": lax.div(q, XN), "x": lax.rem(q, XN)}

    def tp_device(q):
        return {"y": lax.div(q, 2), "c": lax.rem(q, 2)}

    def rows_at(base, size):
        return pl.ds(pl.multiple_of(base, size), size)

    barrier = pltpu.get_barrier_semaphore()
    near = [{"z": zmod(z + 1)}, {"z": zmod(z - 1)}]
    near += [{"x": xmod(x + i)} for i in range(1, XN)]
    near += [tp_device(lax.rem(tp + t, TN)) for t in range(1, TN)]
    for device in near:
        pl.semaphore_signal(barrier, 1, device_id=device, device_id_type=MESH)

    own_rows = rows_at(f * 32, 32)
    loads = [
        pltpu.make_async_copy(src, dst, s_loc.at[n])
        for n, (src, dst) in enumerate(
            (
                (wt_in.at[:, 0:LA], wa.at[own_rows]),
                (wt_in.at[:, LA:1024], wb.at[own_rows]),
                (idx_in, idx_ref),
                (up_in, up_ref),
                (dn_in, dn_ref),
                (tok_in, tok_ref),
                (cot_in, cot_ref),
            )
        )
    ]
    for load in loads:
        load.start()
    loads[0].wait()
    loads[1].wait()
    pl.semaphore_wait(barrier, len(near))

    def wave_on(d, k):
        pl.semaphore_signal(
            wave.at[d, k], 1, device_id=ring_device(d), device_id_type=MESH
        )

    def wave_step(k):
        for d in range(2):
            if k < 8 or d == 0:
                pl.semaphore_wait(wave.at[d, k], 1)
            if k < 7 or (k == 7 and d == 0):
                wave_on(d, k + 1)

    def select(m):
        pick = jnp.where(iota((512, FN), 0) == idx_ref[m : m + 1, :], 1.0, 0.0).astype(BF)
        down = jnp.transpose(nn(dn_ref[...], pick))
        sb32[:, 2 * m, :] = down[:, 0:128]
        sb32[:, 2 * m + 1, :] = down[:, 128:256]
        wide = jnp.concatenate([up32[:, c, :] for c in range(4)], axis=0).astype(BF)
        up = jnp.concatenate([nn(wide, pick), jnp.zeros((64, FN), F32)], axis=0)
        sb32[:, 4 + m, :] = jnp.transpose(up)

    def exchange_start(src, dst, n):
        own = pltpu.make_async_copy(src.at[f, 0:6], dst.at[f, 0:6], l_e.at[n])
        own.start()

        @pl.loop(1, FN, unroll=7)
        def _(p):
            q = lax.rem(f + p, FN)
            remote(src.at[q, 0:6], dst.at[f, 0:6], s_e.at[n], r_e.at[n], plane_device(q)).start()

    def exchange_wait(src, dst, n):
        pltpu.make_async_copy(src.at[f, 0:6], dst.at[f, 0:6], l_e.at[n]).wait()
        remote(
            src.at[0 : FN - 1, 0:6], dst.at[0 : FN - 1, 0:6], s_e.at[n], r_e.at[n], plane_device(f)
        ).wait_recv()

    def exchange_drain(src, dst, n):
        remote(
            src.at[0 : FN - 1, 0:6], dst.at[0 : FN - 1, 0:6], s_e.at[n], r_e.at[n], plane_device(f)
        ).wait_send()

    def a_rows(d, k, xs):
        zz = zmod(z - k) if d == 0 else zmod(z + k)
        return rows_at(zz * 128 + xs * 32, 32)

    def b_rows(d, k):
        return a_rows(d, k, x)

    def ring_device(d):
        return {"z": zmod(z + 1) if d == 0 else zmod(z - 1)}

    def a_copy(d, k, xs):
        rows = wa.at[a_rows(d, k, xs)]
        return remote(rows, rows, s_a.at[d], r_a.at[d, k + 1, xs], ring_device(d))

    def a_wait(d, k, xs):
        rows = wa.at[a_rows(d, k, xs)]
        remote(rows, rows, s_a.at[d], r_a.at[d, k, xs], ring_device(d)).wait_recv()

    def ax_copy(i):
        rows = wa.at[own_rows]
        return remote(rows, rows, s_ax, r_ax.at[x], {"x": xmod(x + i)})

    def ax_wait(xs):
        rows = wa.at[a_rows(0, 0, xs)]
        remote(rows, rows, s_ax, r_ax.at[xs], {"x": xmod(x + 1)}).wait_recv()

    def b_copy(d, k):
        rows = wb.at[b_rows(d, k)]
        return remote(rows, rows, s_b.at[d], r_b.at[d, k + 1], ring_device(d))

    def b_wait(d, k):
        rows = wb.at[b_rows(d, k)]
        remote(rows, rows, s_b.at[d], r_b.at[d, k], ring_device(d)).wait_recv()

    def b_half(d, k):
        zz = zmod(z - k) if d == 0 else zmod(z + k)
        return wb.at[rows_at(zz * 128 + x * 32 + 16 * d, 16)]

    def b_half_copy(d):
        rows = b_half(d, 7)
        return remote(rows, rows, s_b.at[d], r_b.at[d, 8], ring_device(d))

    def b_half_wait(d):
        rows = b_half(d, 8)
        remote(rows, rows, s_b.at[d], r_b.at[d, 8], ring_device(d)).wait_recv()

    def slot(d, k):
        return k if d == 0 else 8 + k

    def x_device(side):
        return {"x": xmod(x + 1)} if side == 0 else {"x": xmod(x - 1)}

    def bx_rows(d, k, from_x):
        return wb.at[a_rows(d, k, from_x)]

    def bx_copy(side, d, k):
        rows = bx_rows(d, k, x)
        n = slot(d, k)
        return remote(rows, rows, s_bx.at[side], r_bx.at[side, n], x_device(side))

    def bx_wait(side, d, k):
        n = slot(d, k)
        rows = bx_rows(d, k, xmod(x - 1) if side == 0 else xmod(x + 1))
        remote(rows, rows, s_bx.at[side], r_bx.at[side, n], x_device(side)).wait_recv()

    def bf_rows(side, d, k, from_x):
        zz = zmod(z - k) if d == 0 else zmod(z + k)
        return wb.at[rows_at(zz * 128 + from_x * 32 + 16 * side, 16)]

    def bf_copy(side, d, k):
        n = slot(d, k)
        rows = bf_rows(side, d, k, xmod(x - 1) if side == 0 else xmod(x + 1))
        return remote(rows, rows, s_bf.at[side], r_bf.at[side, n], x_device(side))

    def bf_wait(side, d, k):
        n = slot(d, k)
        rows = bf_rows(side, d, k, xmod(x + 2))
        remote(rows, rows, s_bf.at[side], r_bf.at[side, n], x_device(side)).wait_recv()

    def b8_copy(d, i):
        rows = b_half(d, 8)
        return remote(rows, rows, s_b8, r_b8.at[d, x], {"x": xmod(x + i)})

    def b8_wait(d, i):
        from_x = xmod(x + i)
        zz = zmod(z + 8)
        rows = wb.at[rows_at(zz * 128 + from_x * 32 + 16 * d, 16)]
        remote(rows, rows, s_b8, r_b8.at[d, from_x], {"x": from_x}).wait_recv()

    def spread(d, k):
        for side in range(2):
            bx_copy(side, d, k).start()

    def forward_x(d, k):
        for side in range(2):
            bx_wait(side, d, k)
            bf_copy(side, d, k).start()

    def complete_x(d, k):
        for side in range(2):
            bf_wait(side, d, k)

    def rs_copy(zz):
        c, h = lax.div(zz, 2), lax.rem(zz, 2)
        return remote(
            rs_send.at[zz], rs_recv.at[tp, h], s_rs, r_rs.at[tp, h], tp_device(c)
        )

    def kv_piece(d, k):
        zz = zmod(z - k) if d == 0 else zmod(z + k)
        c = lax.div(zz, 2)
        rows = rows_at(zz * 128, 128)
        part = nt(tok_ref[:, 0:LA], wa[rows, :]) + nt(tok_ref[:, LA:1024], wb[rows, :])

        @pl.when(c == tp)
        def _():
            own_kv[lax.rem(zz, 2)] = part

        @pl.when(c != tp)
        def _():
            rs_send[zz] = part.astype(BF)
            rs_copy(zz).start()

    def ig_piece(k, j):
        odd = lax.rem(z + k, 2)
        start = zmod(jnp.where(odd == 1, z + k - 1, z - k))
        rows = rows_at(start * 128, 256)
        cot = cot_ref[:, rows]
        if j == 0:
            acc[:, 0:LA] += nn(cot, wa[rows, :])
            acc[:, LA:512] += nn(cot, wb[rows, 0 : 512 - LA])
        else:
            acc[:, 512:1024] += nn(cot, wb[rows, 512 - LA : LB])

    def piece(k, j):
        if j < 2:
            kv_piece(j, k)
        else:
            ig_piece(k, j - 2)

    def block(k):
        for j in range(4):
            piece(k, j)

    rep = jnp.where(lax.div(iota((FN, 1024), 1), 16) == iota((FN, 1024), 0), 1.0, 0.0).astype(BF)
    rep_up = jnp.where(lax.div(iota((FN, 256), 1), 4) == iota((FN, 256), 0), 1.0, 0.0).astype(BF)
    lane16 = lax.rem(iota((16, 1024), 1), 16)
    lane4 = lax.rem(iota((16, 256), 1), 4)
    first = iota((16, 256), 1) < 128
    cot_cols = pl.ds(pl.multiple_of(tp * 256, 256), 256)

    def folded(value):
        return jnp.where(first, value[0:16], value[16:32])

    def unfolded(value):
        return jnp.concatenate(
            [jnp.where(first, value, 0.0), jnp.where(first, 0.0, value)], axis=0
        )

    def adapters():
        exchange_wait(sb1, rb1, 0)
        rb32[...] = rb1[...].astype(F32)
        for m in range(2):
            down, up = arrived(rb32, m)
            wide = nn(down, rep)
            total = jnp.zeros((16, 1024), F32)
            for d in range(16):
                total = jnp.where(lane16 == d, wide[16 * d : 16 * d + 16], total)
            d2t[16 * m : 16 * m + 16] = total.astype(BF)
            wide = nn(up, rep_up)
            total = jnp.zeros((16, 256), F32)
            for d in range(4):
                total = jnp.where(lane4 == d, wide[16 * d : 16 * d + 16], total)
            up2[16 * m : 16 * m + 16] = total.astype(BF)
        ar_send[0:16] = folded(nt(d2t[...], tok_ref[...]))
        ar_send[16:32] = 2.0 * folded(nt(up2[...], cot_ref[:, cot_cols]))
        ar_recv[tp] = ar_send[...]

        @pl.loop(1, TN)
        def _(t):
            ar_copy(t).start()

    def ar_copy(t):
        q = lax.rem(tp + t, TN)
        return remote(ar_send, ar_recv.at[tp], s_ar, r_ar.at[tp], tp_device(q))

    def tiles():
        @pl.loop(1, TN)
        def _(t):
            q = lax.rem(tp + t, TN)
            remote(ar_send, ar_recv.at[q], s_ar, r_ar.at[q], tp_device(q)).wait_recv()

        total = ar_recv[0]
        for q in range(1, TN):
            total = total + ar_recv[q]
        low = unfolded(total[0:16].astype(BF).astype(F32))
        back = unfolded(total[16:32].astype(BF).astype(F32))
        low_t[...] = jnp.transpose(low).astype(BF)
        back_t[...] = jnp.transpose(back).astype(BF)
        low, back = low.astype(BF), back.astype(BF)
        down = nn(back, tok_ref[...])
        up = 2.0 * nn(low, cot_ref[:, cot_cols])
        zeros = jnp.zeros((64, 256), BF)
        for m in range(2):
            mine = down[16 * m : 16 * m + 16]
            wide = jnp.concatenate(
                [jnp.where(lane16 == d, mine, 0.0).astype(BF) for d in range(16)], axis=0
            )
            packed = jnp.transpose(nt(wide, rep))
            sb32[:, 2 * m, :] = packed[:, 0:128]
            sb32[:, 2 * m + 1, :] = packed[:, 128:256]
            mine = up[16 * m : 16 * m + 16]
            wide = jnp.concatenate(
                [jnp.where(lane4 == d, mine, 0.0).astype(BF) for d in range(4)] + [zeros], axis=0
            )
            sb32[:, 4 + m, :] = jnp.transpose(nt(wide, rep_up))
        sb2[...] = sb32[...].astype(BF)
        exchange_start(sb2, rb2, 1)

    for i in range(1, XN):
        ax_copy(i).start()
    for d in range(2):
        b_copy(d, 0).start()
        a_copy(d, 0, x).start()
        wave_on(d, 1)
    spread(0, 0)
    for load in loads[2:5]:
        load.wait()
    up32[...] = up_ref[...].astype(F32)
    sb32[...] = jnp.zeros_like(sb32)

    def ring_b(k):
        for d in range(2):
            b_wait(d, k)

            @pl.when(k < 7)
            def _():
                b_copy(d, k).start()

            @pl.when(k == 7)
            def _():
                b_half_copy(d).start()

            spread(d, k)

    def ring_a(k, i):
        xs = xmod(x + i)
        for d in range(2):
            a_wait(d, k, xs)

            @pl.when((k < 7) | (lax.div(xs, 2) == d))
            def _():
                a_copy(d, k, xs).start()

    wave_step(1)
    select(0)
    wave_step(2)
    for i in range(1, XN):
        xs = xmod(x + i)
        ax_wait(xs)
        for d in range(2):
            a_copy(d, 0, xs).start()
    select(1)
    wave_step(3)
    sb1[...] = sb32[...].astype(BF)
    ring_b(1)
    wave_step(4)
    for i in range(XN):
        ring_a(1, i)
    wave_step(5)
    forward_x(0, 0)
    ring_b(2)
    wave_step(6)
    for i in range(XN):
        ring_a(2, i)
    for d in range(2):
        forward_x(d, 1)
    complete_x(0, 0)
    wave_step(7)
    wave_step(8)
    exchange_start(sb1, rb1, 0)
    acc[...] = jnp.zeros_like(acc)
    loads[5].wait()
    loads[6].wait()

    @pl.loop(3, 8)
    def _(k):
        ring_b(k)
        for i in range(XN):
            ring_a(k, i)

            if i == 0:
                piece(k - 3, i)
            else:

                @pl.when(k >= 4)
                def _():
                    piece(k - 3, i)

        for d in range(2):
            forward_x(d, k - 1)
        for d in range(2):
            complete_x(d, k - 2)

        @pl.when(k == ADAPT_AT)
        def _():
            adapters()

        @pl.when(k == TILES_AT)
        def _():
            tiles()

    piece(5, 0)
    piece(5, 1)
    for d in range(2):
        forward_x(d, 7)
    for d in range(2):
        b_half_wait(d)
        for i in range(1, XN):
            b8_copy(d, i).start()
    for h in range(2):
        for d in range(2):
            a_wait(d, 8, 2 * d + h)
    piece(5, 2)
    piece(5, 3)
    for d in range(2):
        complete_x(d, 6)
    block(6)
    for d in range(2):
        complete_x(d, 7)
    kv_piece(0, 7)
    kv_piece(1, 7)
    for d in range(2):
        for i in range(1, XN):
            b8_wait(d, i)
    kv_piece(0, 8)
    for k in (7, 8):
        for j in range(2):
            ig_piece(k, j)
    ig_ref[...] = (acc[...] + nn(back_t[...], d2t[...]).astype(BF).astype(F32)).astype(BF)
    kvl = (2.0 * nn(low_t[...], up2[...])).astype(BF).astype(F32)
    exchange_wait(sb2, rb2, 1)
    got_ref[...] = rb2[...]
    ids_ref[...] = idx_ref[...]

    for h in range(2):
        cols = slice(128 * h, 128 * h + 128)
        total = own_kv[h]
        for t in range(1, TN):
            q = lax.rem(tp + t, TN)
            remote(
                rs_send.at[0], rs_recv.at[q, h], s_rs, r_rs.at[q, h], tp_device(q)
            ).wait_recv()
            total = total + rs_recv[q, h].astype(F32)
        kv_ref[:, cols] = (total + kvl[:, cols]).astype(BF)

    def drain(ref, sem):
        remote(ref, ref, sem, s_loc.at[0], ring_device(0)).wait_send()

    exchange_drain(sb1, rb1, 0)
    exchange_drain(sb2, rb2, 1)
    drain(wa.at[0:96], s_ax)
    drain(wb.at[0:96], s_b8)
    drain(ar_recv.at[0 : TN - 1], s_ar)
    drain(rs_send.at[0 : 2 * TN - 2], s_rs)
    for d in range(2):
        drain(wa.at[0:960], s_a.at[d])
        drain(wb.at[0:240], s_b.at[d])
        drain(wb.at[0:480], s_bx.at[d])
        drain(wb.at[0:240], s_bf.at[d])


def fused(tok, wt, cot, idx, dn, up):
    dma = pltpu.SemaphoreType.DMA
    vmem = pl.BlockSpec(memory_space=pltpu.VMEM)
    kv, ig, got, ids = pl.pallas_call(
        kernel,
        out_shape=(
            jax.ShapeDtypeStruct((256, 256), BF),
            jax.ShapeDtypeStruct((256, 1024), BF),
            jax.ShapeDtypeStruct((FN, 8, 128), BF),
            jax.ShapeDtypeStruct((2, FN), jnp.int32),
        ),
        in_specs=[pl.BlockSpec(memory_space=pltpu.HBM)] * 6,
        out_specs=[vmem] * 4,
        scratch_shapes=[
            pltpu.VMEM((2048, LA), BF),
            pltpu.VMEM((2048, LB), BF),
            pltpu.VMEM((256, 1024), F32),
            pltpu.VMEM((2, 256, 128), F32),
            pltpu.VMEM((ZN, 256, 128), BF),
            pltpu.VMEM((TN, 2, 256, 128), BF),
            pltpu.VMEM((256, 32), BF),
            pltpu.VMEM((256, 32), BF),
            pltpu.VMEM((256, 1024), BF),
            pltpu.VMEM((256, 2048), BF),
            pltpu.VMEM((2, FN), jnp.int32),
            pltpu.VMEM((256, 512), BF),
            pltpu.VMEM((16, 4, 512), BF),
            pltpu.VMEM((16, 4, 512), F32),
            pltpu.VMEM((FN, 8, 128), F32),
            pltpu.VMEM((FN, 8, 128), BF),
            pltpu.VMEM((FN, 8, 128), BF),
            pltpu.VMEM((FN, 8, 128), F32),
            pltpu.VMEM((FN, 8, 128), BF),
            pltpu.VMEM((FN, 8, 128), BF),
            pltpu.VMEM((32, 1024), BF),
            pltpu.VMEM((32, 256), BF),
            pltpu.VMEM((32, 256), F32),
            pltpu.VMEM((TN, 32, 256), F32),
            pltpu.SemaphoreType.REGULAR((2, 9)),
            dma(()),
            dma((2, XN)),
            dma((7,)),
            dma((2,)),
            dma((2, 9, XN)),
            dma(()),
            dma((XN,)),
            dma((2,)),
            dma((2, 9)),
            dma((2,)),
            dma((2, 16)),
            dma((2,)),
            dma((2, 16)),
            dma(()),
            dma((TN, 2)),
            dma(()),
            dma((TN,)),
            dma((2,)),
            dma((2,)),
            dma((2,)),
        ],
        compiler_params=pltpu.CompilerParams(
            collective_id=0, has_side_effects=True, vmem_limit_bytes=32 << 20
        ),
    )(*(pltpu.with_memory_space_constraint(v, pltpu.HBM) for v in (tok, wt, cot, idx, dn, up)))
    return pl.pallas_call(
        finish,
        out_shape=(
            jax.ShapeDtypeStruct((256, 256), BF),
            jax.ShapeDtypeStruct((256, 1024), BF),
            jax.ShapeDtypeStruct((256, 512), F32),
            jax.ShapeDtypeStruct((16, 4, 512), F32),
        ),
        in_specs=[vmem] * 4,
        out_specs=[vmem] * 4,
        scratch_shapes=[pltpu.VMEM((FN, 8, 128), F32)],
        compiler_params=pltpu.CompilerParams(vmem_limit_bytes=16 << 20),
    )(kv, ig, got, ids)


def local(tokens, frozen_weight, cotangent, block_adapter_index, down_weight, up_weight):
    tok = tokens.reshape(256, 1024)
    cot = cotangent.reshape(256, 2048)
    wt = frozen_weight.T
    dn = down_weight.transpose(1, 2, 0).reshape(256, 512)
    up = up_weight.transpose(1, 2, 0)
    kv, ig, gd, gu = fused(tok, wt, cot, block_adapter_index, dn, up)
    return (
        kv.reshape(2, 128, 256),
        ig.reshape(2, 128, 1024),
        gd.reshape(16, 16, 512).transpose(2, 0, 1),
        gu.transpose(2, 0, 1),
    )


def solution(mesh):
    finer = Mesh(mesh.devices.reshape(ZN, XN, 4, 2), ("z", "x", "y", "c"))
    return jax.shard_map(
        local,
        mesh=finer,
        in_specs=(
            P(None, PLANE, TP),
            P(TP, PLANE),
            P(None, PLANE, None),
            P(),
            P(None, ALL, None),
            P(None, None, ALL),
        ),
        out_specs=(
            P(None, PLANE, TP),
            P(None, PLANE, TP),
            P(None, ALL, None),
            P(None, None, ALL),
        ),
        check_vma=False,
    )
```
